32 devices in a mesh: grp: 1 (over z), comp: 4 (over y), row: 8 (over x, core).
Axes of the slice: x: 4, y: 4, z: 1, core: 2. Of those that a mesh axis runs over, the one named last changes fastest.
The devices are a block of a 4x4x8 slice.
Arguments:
- points: bfloat16 [2048, 256], P(('grp', 'row'))
- mu_init: float32 [2, 16384, 128], P(None, ('grp', 'comp'))
- logpi_init: float32 [2, 16384], P(None, ('grp', 'comp'))
- inv_temp: float32 [3], replicated
Outputs:
- output 1: float32 [2, 16384, 128], P(None, ('grp', 'comp'))
- output 2: float32 [2, 16384], P(None, ('grp', 'comp'))
- output 3: float32 [2, 2048], P(None, ('grp', 'row'))
All inputs are finite; a program needn't handle non-finite values.
Results may differ from the reference program's by a relative error of at most 0.00128443.
Values are sent between devices in bfloat16 or wider.
A program may use at most 768 MiB of HBM per device.

```python
import jax
import jax.numpy as jnp
from jax import lax

POINTS = 2048
DIM = 256
HALF = 128
COMPS = 16384
SWEEPS = 3
CLUSTERS = 32
BLOCK = 256

EPS_COUNT = 1e-6
PRIOR_ALPHA = 1e-3


def setup_inputs(seed: int = 0, part: int = 0) -> dict:
    base_key = jax.random.key(seed)
    part_key = jax.random.fold_in(base_key, part)
    key_c, key_x, key_j, key_m, key_w = jax.random.split(part_key, 5)
    key_b = jax.random.fold_in(base_key, 1000)
    centers = jax.random.normal(key_c, (2, CLUSTERS, HALF), jnp.float32)
    source = (jnp.arange(POINTS) * CLUSTERS) // POINTS
    noise_x = jax.random.normal(key_x, (2, POINTS, HALF), jnp.float32)
    pts_pair = centers[:, source, :] + 0.7 * noise_x
    points = jnp.transpose(pts_pair, (1, 0, 2)).reshape(POINTS, DIM).astype(jnp.bfloat16)
    pick_ids = jax.random.randint(key_j, (2, COMPS), 0, CLUSTERS)
    noise_m = jax.random.normal(key_m, (2, COMPS, HALF), jnp.float32)
    mu_init = centers[jnp.arange(2)[:, None], pick_ids] + 0.5 * noise_m
    raw_logit = jax.random.normal(key_w, (2, COMPS), jnp.float32)
    logpi_init = raw_logit - jax.nn.logsumexp(raw_logit, axis=1, keepdims=True)
    inv_temp = (0.5 + 1.5 * jax.random.uniform(key_b, (SWEEPS,), jnp.float32)) / HALF
    return {"points": points, "mu_init": mu_init, "logpi_init": logpi_init, "inv_temp": inv_temp}


def reference(points, mu_init, logpi_init, inv_temp):
    x_blocks = points.astype(jnp.float32).reshape(POINTS // BLOCK, BLOCK, 2, HALF)
    x_blocks = jnp.transpose(x_blocks, (0, 2, 1, 3))
    sq_blocks = jnp.sum(x_blocks * x_blocks, axis=3)

    def one_sweep(carry_in, beta_t):
        mean_vecs, log_wts = carry_in
        mu_round = mean_vecs.astype(jnp.bfloat16).astype(jnp.float32)
        mu_sq = jnp.sum(mean_vecs * mean_vecs, axis=2)

        def point_block(acc_pair, block_in):
            x_block, sq_norm = block_in
            cross_dot = jnp.einsum("snh,skh->snk", x_block, mu_round)
            logits = log_wts[:, None, :] - beta_t * (sq_norm[:, :, None] - 2.0 * cross_dot + mu_sq[:, None, :])
            row_max = jnp.max(logits, axis=2)
            shifted = jnp.exp(logits - row_max[:, :, None])
            row_sum = jnp.sum(shifted, axis=2)
            resp_f = shifted / row_sum[:, :, None]
            log_norm = row_max + jnp.log(row_sum)
            resp_round = resp_f.astype(jnp.bfloat16).astype(jnp.float32)
            stat_part = jnp.einsum("snk,snh->skh", resp_round, x_block)
            count_acc, stat_acc = acc_pair
            return (count_acc + jnp.sum(resp_f, axis=1), stat_acc + stat_part), log_norm

        zero_acc = (jnp.zeros((2, COMPS), jnp.float32), jnp.zeros((2, COMPS, HALF), jnp.float32))
        (counts, stat_sum), norm_blocks = lax.scan(point_block, zero_acc, (x_blocks, sq_blocks))
        new_means = stat_sum / (counts[:, :, None] + EPS_COUNT)
        new_logw = jnp.log((counts + PRIOR_ALPHA) / (POINTS + COMPS * PRIOR_ALPHA))
        return (new_means, new_logw), norm_blocks

    (mean_vecs, log_wts), norm_all = lax.scan(one_sweep, (mu_init, logpi_init), inv_temp)
    log_norm = jnp.transpose(norm_all[-1], (1, 0, 2)).reshape(2, POINTS)
    return mean_vecs, log_wts, log_norm
```

```python
import functools
import math

import jax
import jax.numpy as jnp
from jax import lax
from jax.experimental import pallas as pl
from jax.experimental.pallas import tpu as pltpu
from jax.sharding import PartitionSpec as P

EPS_COUNT = 1e-6
PRIOR_ALPHA = 1e-3
LOG2E = math.log2(math.e)
LN2 = math.log(2.0)
LANES = 128
MESH = pl.DeviceIdType.MESH
NT = (((1,), (1,)), ((), ()))


def em_kernel(dims, beta_ref, x_ref, mu_hbm, logpi_ref, o_mu, o_small,
              xg, mu_f, mu_b, a_bc, lbuf, rb, s_acc, n_acc, mloc, stat_src, stat_buf,
              mu_all, small_src, small_buf,
              loc_sem, out_sem, x_send, x_recv, st_send, st_recv, sm_send, sm_recv,
              ag_send, ag_recv, sib_send, sib_recv):
    fits, n_comp, n_row, sweeps = dims["fits"], dims["comp"], dims["row"], dims["sweeps"]
    n_rows, half = x_ref.shape[0], mu_f.shape[1]
    nx = n_row // fits
    kd = mu_f.shape[0]
    cp = n_rows * fits
    lb = cp // LANES
    n_peer = n_comp * nx
    pieces = dims["pieces"]
    kp = kd // pieces
    total_pts = n_rows * n_row
    total_comp = kd * nx * n_comp

    grp = lax.axis_index("grp")
    comp = lax.axis_index("comp")
    row = lax.axis_index("row")
    fit = lax.rem(row, fits)
    xi = row // fits
    me = comp * nx + xi

    def dev(c, r):
        return (grp, c, r)

    def stat_peer(k):
        d_c, d_x = k // nx, k % nx
        return lax.rem(comp + d_c, n_comp), lax.rem(xi + d_x, nx)

    mu_cp = pltpu.make_async_copy(mu_hbm.at[fit, pl.ds(pl.multiple_of(xi * kd, kd), kd), :], mu_f, loc_sem)
    mu_cp.start()

    barrier = pltpu.get_barrier_semaphore()
    n_sig = 0
    for k in range(1, n_peer):
        c, x = stat_peer(k)
        pl.semaphore_signal(barrier, inc=1, device_id=dev(c, x * fits + fit), device_id_type=MESH)
        n_sig += 1
    for k in range(nx):
        for f in range(1, fits):
            x = lax.rem(xi + k, nx)
            pl.semaphore_signal(barrier, inc=1, device_id=dev(comp, x * fits + lax.rem(fit + f, fits)), device_id_type=MESH)
            n_sig += 1
    pl.semaphore_wait(barrier, n_sig)

    def x_cols(f):
        return pl.ds(pl.multiple_of(f * half, half), half)

    my_rows = pl.ds(pl.multiple_of(fit * n_rows, n_rows), n_rows)
    x_copies = []
    for k in (0, 1, 3, 2) if nx == 4 else range(nx):
        for f in range(fits):
            if k == 0 and f == 0:
                continue
            x = lax.rem(xi + k, nx)
            ft = lax.rem(fit + f, fits)
            cpy = pltpu.make_async_remote_copy(
                src_ref=x_ref.at[:, x_cols(ft)],
                dst_ref=xg.at[xi, my_rows],
                send_sem=x_send, recv_sem=x_recv.at[xi],
                device_id=dev(comp, x * fits + ft), device_id_type=MESH)
            cpy.start()
            x_copies.append(cpy)
    xg[xi, my_rows, :] = x_ref[:, x_cols(fit)]

    def comp_terms(t, rows, mu, logw):
        beta = beta_ref[t]
        sq = jnp.sum(mu * mu, axis=1, keepdims=True)
        a = (logw - beta * sq) * LOG2E
        a_bc[rows, :] = jnp.broadcast_to(a, (a.shape[0], LANES))
        mu_b[rows, :] = mu.astype(jnp.bfloat16)

    mu_cp.wait()
    for b in range(kd // LANES):
        rows = pl.ds(b * LANES, LANES)
        lw = logpi_ref[:, pl.ds(pl.multiple_of(xi * kd + b * LANES, LANES), LANES)]
        pick = lax.broadcasted_iota(jnp.int32, (fits, LANES), 0) == fit
        lw = jnp.sum(jnp.where(pick, lw, 0.0), axis=0, keepdims=True)
        lw = jnp.transpose(jnp.broadcast_to(lw, (LANES, LANES)))
        comp_terms(0, rows, mu_f[rows, :], lw[:, 0:1])

    def lanes_tile(v):
        return jnp.concatenate([v] * lb, axis=1)

    KB = 128
    nkb = kd // KB

    def e_chunk(t, q):
        c2 = beta_ref[t] * (2.0 * LOG2E)
        lbuf[q] = lax.dot_general(mu_b[...], xg[q], NT, preferred_element_type=jnp.float32)

        def pass1(b, m8):
            rows = pl.ds(pl.multiple_of(b * KB, KB), KB)
            l = lbuf[q, rows, :] * c2 + lanes_tile(a_bc[rows, :])
            lbuf[q, rows, :] = l
            return jnp.maximum(m8, jnp.max(l.reshape(KB // 8, 8, cp), axis=0))

        m8 = lax.fori_loop(0, nkb, pass1, jnp.full((8, cp), -jnp.inf, jnp.float32))
        m = jnp.max(m8, axis=0, keepdims=True)

        def pass2(b, r8):
            rows = pl.ds(pl.multiple_of(b * KB, KB), KB)
            p = jnp.exp2(lbuf[q, rows, :] - m)
            lbuf[q, rows, :] = p
            return r8 + jnp.sum(p.reshape(KB // 8, 8, cp), axis=0)

        r8 = lax.fori_loop(0, nkb, pass2, jnp.zeros((8, cp), jnp.float32))
        r = jnp.sum(r8, axis=0, keepdims=True)
        for j in range(lb):
            cols = slice(j * LANES, (j + 1) * LANES)
            for ref in (stat_src.at[t, q], stat_buf.at[t, q, me]):
                ref[0, j:j + 1, :] = m[:, cols]
                ref[1, j:j + 1, :] = r[:, cols]

    def stat_copy(t, q, k):
        c, x = stat_peer(k)
        return pltpu.make_async_remote_copy(
            src_ref=stat_src.at[t, q], dst_ref=stat_buf.at[t, q, me],
            send_sem=st_send.at[t, q], recv_sem=st_recv.at[t, q],
            device_id=dev(c, x * fits + fit), device_id_type=MESH)

    def stat_start(t, q):
        for k in range(1, n_peer):
            stat_copy(t, q, k).start()

    def stat_wait(t, q, send):
        part = stat_buf.at[t, q, pl.ds(0, n_peer - 1)]
        d = pltpu.make_async_copy(part, part, st_send.at[t, q] if send else st_recv.at[t, q])
        d.wait()

    def scale_of(t, q):
        m_all = stat_buf[t, q, :, 0]
        r_all = stat_buf[t, q, :, 1]
        m = jnp.max(m_all, axis=0)
        r = jnp.sum(r_all * jnp.exp2(m_all - m), axis=0)
        return m, r, jnp.exp2(stat_src[t, q, 0] - m) / r

    def m_rows(q, rows, nrow, sc):
        sc_row = jnp.concatenate([jnp.broadcast_to(sc[j:j + 1, :], (nrow, LANES)) for j in range(lb)], axis=1)
        res = lbuf[q, rows, :] * sc_row
        cnt = res[:, 0:LANES]
        for j in range(1, lb):
            cnt = cnt + res[:, j * LANES:(j + 1) * LANES]
        rb[rows, :] = res.astype(jnp.bfloat16)
        return cnt

    def m_chunk(t, q, first):
        m, r, sc = scale_of(t, q)

        def body(b, carry):
            rows = pl.ds(pl.multiple_of(b * KB, KB), KB)
            cnt = m_rows(q, rows, KB, sc)
            n_acc[rows, :] = jnp.where(first, cnt, n_acc[rows, :] + cnt)
            return carry

        lax.fori_loop(0, nkb, body, 0)
        s = jnp.dot(rb[...], xg[q], preferred_element_type=jnp.float32)
        s_acc[...] = jnp.where(first, s, s_acc[...] + s)
        return m, r

    order = (0, 1, 3, 2) if nx == 4 else tuple(range(nx))
    for off in order:
        q = lax.rem(xi + off, nx)
        n_in = (fits - 1) if off == 0 else fits
        part = xg.at[q, pl.ds(0, n_in * n_rows)]
        pltpu.make_async_copy(part, part, x_recv.at[q]).wait()
        e_chunk(0, q)
        stat_start(0, q)

    def sweep(t, carry):
        def m_body(q, c):
            stat_wait(t, q, False)
            m_chunk(t, q, q == 0)
            return c

        lax.fori_loop(0, nx, m_body, 0)

        def terms(b, c):
            rows = pl.ds(pl.multiple_of(b * KB, KB), KB)
            cnt = jnp.sum(n_acc[rows, :], axis=1, keepdims=True)
            mu = s_acc[rows, :] / (cnt + EPS_COUNT)
            logw = jnp.log((cnt + PRIOR_ALPHA) / (total_pts + total_comp * PRIOR_ALPHA))
            comp_terms(t + 1, rows, mu, logw)
            return c

        lax.fori_loop(0, nkb, terms, 0)

        def e_body(q, c):
            e_chunk(t + 1, q)
            stat_start(t + 1, q)
            return c

        lax.fori_loop(0, nx, e_body, 0)
        return carry

    lax.fori_loop(0, sweeps - 1, sweep, 0)

    tl = sweeps - 1

    sq_rows = []
    for j in range(lb):
        xb = xg[xi, j * LANES:(j + 1) * LANES, :].astype(jnp.float32)
        sq_rows.append(jnp.sum(jnp.transpose(xb * xb), axis=0, keepdims=True))
    sq = jnp.concatenate(sq_rows, axis=0)

    def m_last(q, c):
        stat_wait(tl, q, False)
        m, r = m_chunk(tl, q, q == 0)
        return c

    lax.fori_loop(0, nx, m_last, 0)
    m, r, _ = scale_of(tl, xi)
    small_src[1, 0:lb, :] = m * LN2 + jnp.log(r) - beta_ref[tl] * sq

    right = lax.rem(xi + 1, nx)
    left = lax.rem(xi + nx - 1, nx)
    far = lax.rem(xi + 2, nx)
    sib = xi * fits + lax.rem(fit + 1, fits)

    def span(x, p):
        return pl.ds(pl.multiple_of(x * kd + p * kp, kp), kp)

    def mu_copy(x, p, send_sem, recv_sem, r):
        part = mu_all.at[fit, span(x, p)]
        return pltpu.make_async_remote_copy(src_ref=part, dst_ref=part, send_sem=send_sem, recv_sem=recv_sem,
                                            device_id=dev(comp, r), device_id_type=MESH)

    def out_copy(f, x, p):
        return pltpu.make_async_copy(mu_all.at[f, span(x, p)], o_mu.at[f, span(x, p)], out_sem)

    waits = []
    half_p = pieces // 2
    porder = [p // 2 + (p % 2) * half_p for p in range(pieces)]
    for p in porder:
        for b in range(kp // LANES):
            rows = pl.ds(p * kp + b * LANES, LANES)
            na = n_acc[rows, :]
            cnt = jnp.sum(na, axis=1, keepdims=True)
            mu_all[fit, pl.ds(pl.multiple_of(xi * kd + p * kp + b * LANES, LANES), LANES), :] = s_acc[rows, :] / (cnt + EPS_COUNT)
            n_row_v = jnp.sum(jnp.transpose(na), axis=0, keepdims=True)
            j = p * (kp // LANES) + b
            small_src[0, j:j + 1, :] = jnp.log((n_row_v + PRIOR_ALPHA) / (total_pts + total_comp * PRIOR_ALPHA))
        to_r = mu_copy(xi, p, ag_send.at[0, p], ag_recv.at[0, p], right * fits + fit)
        to_l = mu_copy(xi, p, ag_send.at[1, p], ag_recv.at[1, p], left * fits + fit)
        to_s = mu_copy(xi, p, sib_send.at[0, p], sib_recv.at[0, p], sib)
        to_r.start()
        to_l.start()
        to_s.start()
        oc = out_copy(fit, xi, p)
        oc.start()
        waits += [to_r.wait_send, to_l.wait_send, to_s.wait_send, oc.wait]

    sm_me = small_buf.at[row]
    sm_copies = []
    for k in range(1, n_row):
        r = lax.rem(row + k, n_row)
        cpy = pltpu.make_async_remote_copy(src_ref=small_src, dst_ref=sm_me, send_sem=sm_send, recv_sem=sm_recv,
                                           device_id=dev(comp, r), device_id_type=MESH)
        cpy.start()
        sm_copies.append(cpy)
    small_buf[row] = small_src[...]

    for i, p in enumerate(porder):
        for side, src in ((0, left), (1, right)):
            mu_copy(src, p, ag_send.at[2, p], ag_recv.at[side, p], sib).wait_recv()
            if (p < half_p) == (side == 0):
                fw = mu_copy(src, p, ag_send.at[2, p], ag_recv.at[2, p],
                             (right if side == 0 else left) * fits + fit)
                fw.start()
                waits.append(fw.wait_send)
            d = 1 if side == 0 else 3
            ts = mu_copy(src, p, sib_send.at[d, p], sib_recv.at[d, p], sib)
            ts.start()
            oc = out_copy(fit, src, p)
            oc.start()
            waits += [ts.wait_send, oc.wait]
    for p in porder:
        mu_copy(far, p, ag_send.at[2, p], ag_recv.at[2, p], sib).wait_recv()
        ts = mu_copy(far, p, sib_send.at[2, p], sib_recv.at[2, p], sib)
        ts.start()
        oc = out_copy(fit, far, p)
        oc.start()
        waits += [ts.wait_send, oc.wait]
    ofit = lax.rem(fit + 1, fits)
    for d, src in ((0, xi), (1, left), (3, right), (2, far)):
        for p in porder:
            part = mu_all.at[ofit, span(src, p)]
            pltpu.make_async_copy(part, part, sib_recv.at[d, p]).wait()
            oc = out_copy(ofit, src, p)
            oc.start()
            waits.append(oc.wait)

    part = small_buf.at[pl.ds(0, n_row - 1)]
    pltpu.make_async_copy(part, part, sm_recv).wait()
    pltpu.make_async_copy(part, part, sm_send).wait()
    o_small[...] = small_buf[...]
    for w in waits:
        w()
    def drain(t, c):
        for q in range(nx):
            stat_wait(t, q, True)
        return c
    lax.fori_loop(0, sweeps, drain, 0)
    for cpy in x_copies:
        cpy.wait_send()


def solution(mesh):
    comp_size = mesh.shape["comp"]
    row_size = mesh.shape["row"]

    def local_fit(x_local, mu_init, logpi_init, inv_temp):
        n_rows, full_dim = x_local.shape
        fits, n_local, half = mu_init.shape
        sweeps = inv_temp.shape[0]
        nx = row_size // fits
        kd = n_local // nx
        cp = n_rows * fits
        n_peer = comp_size * nx
        pieces = 4
        dims = {"fits": fits, "comp": comp_size, "row": row_size, "sweeps": sweeps, "pieces": pieces}
        f32, bf16 = jnp.float32, jnp.bfloat16
        dma = pltpu.SemaphoreType.DMA
        srows = cp // LANES
        mu, small = pl.pallas_call(
            functools.partial(em_kernel, dims),
            out_shape=(jax.ShapeDtypeStruct((fits, n_local, half), f32),
                       jax.ShapeDtypeStruct((row_size, 2, kd // LANES, LANES), f32)),
            in_specs=[pl.BlockSpec(memory_space=pltpu.SMEM),
                      pl.BlockSpec(memory_space=pltpu.VMEM),
                      pl.BlockSpec(memory_space=pl.ANY),
                      pl.BlockSpec(memory_space=pltpu.VMEM)],
            out_specs=(pl.BlockSpec(memory_space=pl.ANY),
                       pl.BlockSpec(memory_space=pltpu.VMEM)),
            scratch_shapes=[
                pltpu.VMEM((nx, cp, half), bf16),
                pltpu.VMEM((kd, half), f32),
                pltpu.VMEM((kd, half), bf16),
                pltpu.VMEM((kd, LANES), f32),
                pltpu.VMEM((nx, kd, cp), f32),
                pltpu.VMEM((kd, cp), bf16),
                pltpu.VMEM((kd, half), f32),
                pltpu.VMEM((kd, LANES), f32),
                pltpu.VMEM((8, LANES), f32),
                pltpu.VMEM((sweeps, nx, 2, srows, LANES), f32),
                pltpu.VMEM((sweeps, nx, n_peer, 2, srows, LANES), f32),
                pltpu.VMEM((fits, n_local, half), f32),
                pltpu.VMEM((2, kd // LANES, LANES), f32),
                pltpu.VMEM((row_size, 2, kd // LANES, LANES), f32),
                dma, dma, dma, dma((nx,)),
                dma((sweeps, nx)), dma((sweeps, nx)),
                dma, dma,
                dma((3, pieces)), dma((3, pieces)), dma((4, pieces)), dma((4, pieces)),
            ],
            compiler_params=pltpu.CompilerParams(collective_id=0, has_side_effects=True,
                                                 vmem_limit_bytes=60 * 1024 * 1024),
        )(inv_temp, x_local, mu_init, logpi_init)
        row = lax.axis_index("row")
        xi = row // fits
        small = small.reshape(nx, fits, 2, kd // LANES, LANES)
        log_wts = jnp.transpose(small[:, :, 0], (1, 0, 2, 3)).reshape(fits, n_local)
        own = lax.dynamic_index_in_dim(small, xi, 0, keepdims=False)[:, 1]
        per = n_rows // LANES
        lse = lax.dynamic_slice_in_dim(own, lax.rem(row, fits) * per, per, 1).reshape(fits, n_rows)
        return mu, log_wts, lse

    return jax.shard_map(
        local_fit,
        mesh=mesh,
        in_specs=(P(("grp", "row"), None), P(None, ("grp", "comp"), None), P(None, ("grp", "comp")), P()),
        out_specs=(P(None, ("grp", "comp"), None), P(None, ("grp", "comp")), P(None, ("grp", "row"))),
        check_vma=False,
    )
```

```python
import functools
import math

import jax
import jax.numpy as jnp
from jax import lax
from jax.experimental import pallas as pl
from jax.experimental.pallas import tpu as pltpu
from jax.sharding import PartitionSpec as P

EPS_COUNT = 1e-6
PRIOR_ALPHA = 1e-3
LOG2E = math.log2(math.e)
LN2 = math.log(2.0)
LANES = 128
MESH = pl.DeviceIdType.MESH
NT = (((1,), (1,)), ((), ()))


def em_kernel(dims, beta_hbm, x_hbm, mu_hbm, logpi_hbm, mu_all, small_buf,
              beta_ref, x_ref, logpi_ref, xg, mu_f, mu_b, a_bc, lbuf, rb, s_acc, n_acc,
              stat_src, stat_buf, small_src,
              loc_sem, x_send, x_recv, st_send, st_recv, sm_send, sm_recv,
              ag_send, ag_recv, sib_send, sib_recv):
    fits, n_comp, n_row, sweeps = dims["fits"], dims["comp"], dims["row"], dims["sweeps"]
    n_rows, half = x_ref.shape[0], mu_f.shape[1]
    nx = n_row // fits
    kd = mu_f.shape[0]
    cp = n_rows * fits
    lb = cp // LANES
    n_peer = n_comp * nx
    pieces = dims["pieces"]
    kp = kd // pieces
    total_pts = n_rows * n_row
    total_comp = kd * nx * n_comp

    grp = lax.axis_index("grp")
    comp = lax.axis_index("comp")
    row = lax.axis_index("row")
    fit = lax.rem(row, fits)
    xi = row // fits
    me = comp * nx + xi

    def dev(c, r):
        return (grp, c, r)

    def stat_peer(k):
        d_c, d_x = k // nx, k % nx
        return lax.rem(comp + d_c, n_comp), lax.rem(xi + d_x, nx)

    barrier = pltpu.get_barrier_semaphore()
    n_sig = 0
    for k in range(1, n_peer):
        c, x = stat_peer(k)
        pl.semaphore_signal(barrier, inc=1, device_id=dev(c, x * fits + fit), device_id_type=MESH)
        n_sig += 1
    for k in range(nx):
        for f in range(1, fits):
            x = lax.rem(xi + k, nx)
            pl.semaphore_signal(barrier, inc=1, device_id=dev(comp, x * fits + lax.rem(fit + f, fits)), device_id_type=MESH)
            n_sig += 1

    loads = [pltpu.make_async_copy(x_hbm, x_ref, loc_sem.at[0]),
             pltpu.make_async_copy(mu_hbm.at[fit, pl.ds(pl.multiple_of(xi * kd, kd), kd), :], mu_f, loc_sem.at[1]),
             pltpu.make_async_copy(logpi_hbm, logpi_ref, loc_sem.at[2]),
             pltpu.make_async_copy(beta_hbm, beta_ref, loc_sem.at[3])]
    for cpy in loads:
        cpy.start()

    def comp_terms(t, rows, mu, logw):
        beta = beta_ref[t]
        sq = jnp.sum(mu * mu, axis=1, keepdims=True)
        a = (logw - beta * sq) * LOG2E
        a_bc[rows, :] = jnp.broadcast_to(a, (a.shape[0], LANES))
        mu_b[rows, :] = mu.astype(jnp.bfloat16)

    for cpy in loads:
        cpy.wait()
    for b in range(kd // LANES):
        rows = pl.ds(b * LANES, LANES)
        lw = logpi_ref[:, pl.ds(pl.multiple_of(xi * kd + b * LANES, LANES), LANES)]
        pick = lax.broadcasted_iota(jnp.int32, (fits, LANES), 0) == fit
        lw = jnp.sum(jnp.where(pick, lw, 0.0), axis=0, keepdims=True)
        lw = jnp.transpose(jnp.broadcast_to(lw, (LANES, LANES)))
        comp_terms(0, rows, mu_f[rows, :], lw[:, 0:1])

    with jax.named_scope("bar"):
        pl.semaphore_wait(barrier, n_sig)

    def x_cols(f):
        return pl.ds(pl.multiple_of(f * half, half), half)

    my_rows = pl.ds(pl.multiple_of(fit * n_rows, n_rows), n_rows)
    x_copies = []
    for k in (0, 1, 3, 2) if nx == 4 else range(nx):
        for f in range(fits):
            if k == 0 and f == 0:
                continue
            x = lax.rem(xi + k, nx)
            ft = lax.rem(fit + f, fits)
            cpy = pltpu.make_async_remote_copy(
                src_ref=x_ref.at[:, x_cols(ft)],
                dst_ref=xg.at[xi, my_rows],
                send_sem=x_send, recv_sem=x_recv.at[xi],
                device_id=dev(comp, x * fits + ft), device_id_type=MESH)
            cpy.start()
            x_copies.append(cpy)
    xg[xi, my_rows, :] = x_ref[:, x_cols(fit)]

    def lanes_tile(v):
        return jnp.concatenate([v] * lb, axis=1)

    KB = 128
    nkb = kd // KB

    def e_dot(q):
        with jax.named_scope("edot"):
            lbuf[q] = lax.dot_general(mu_b[...], xg[q], NT, preferred_element_type=jnp.float32)

    def e_soft(t, q):
        c2 = beta_ref[t] * (2.0 * LOG2E)
        m8 = jnp.full((8, cp), -jnp.inf, jnp.float32)
        for b in range(nkb):
            rows = slice(b * KB, (b + 1) * KB)
            l = lbuf[q, rows, :] * c2 + lanes_tile(a_bc[rows, :])
            lbuf[q, rows, :] = l
            m8 = jnp.maximum(m8, jnp.max(l.reshape(KB // 8, 8, cp), axis=0))
        m = jnp.max(m8, axis=0, keepdims=True)
        r8 = jnp.zeros((8, cp), jnp.float32)
        for b in range(nkb):
            rows = slice(b * KB, (b + 1) * KB)
            p = jnp.exp2(lbuf[q, rows, :] - m)
            lbuf[q, rows, :] = p
            r8 = r8 + jnp.sum(p.reshape(KB // 8, 8, cp), axis=0)
        r = jnp.sum(r8, axis=0, keepdims=True)
        for j in range(lb):
            cols = slice(j * LANES, (j + 1) * LANES)
            for ref in (stat_src.at[t, q], stat_buf.at[t, q, me]):
                ref[0, j:j + 1, :] = m[:, cols]
                ref[1, j:j + 1, :] = r[:, cols]

    def stat_copy(t, q, k):
        c, x = stat_peer(k)
        return pltpu.make_async_remote_copy(
            src_ref=stat_src.at[t, q], dst_ref=stat_buf.at[t, q, me],
            send_sem=st_send.at[t, q], recv_sem=st_recv.at[t, q],
            device_id=dev(c, x * fits + fit), device_id_type=MESH)

    def stat_start(t, q):
        for k in range(1, n_peer):
            stat_copy(t, q, k).start()

    def stat_wait(t, q, send):
        part = stat_buf.at[t, q, pl.ds(0, n_peer - 1)]
        d = pltpu.make_async_copy(part, part, st_send.at[t, q] if send else st_recv.at[t, q])
        with jax.named_scope("stwait"):
            d.wait()

    def scale_of(t, q):
        m_all = stat_buf[t, q, :, 0]
        r_all = stat_buf[t, q, :, 1]
        m = jnp.max(m_all, axis=0)
        r = jnp.sum(r_all * jnp.exp2(m_all - m), axis=0)
        return m, r, jnp.exp2(stat_src[t, q, 0] - m) / r

    def m_rows(q, rows, nrow, sc):
        sc_row = jnp.concatenate([jnp.broadcast_to(sc[j:j + 1, :], (nrow, LANES)) for j in range(lb)], axis=1)
        res = lbuf[q, rows, :] * sc_row
        cnt = res[:, 0:LANES]
        for j in range(1, lb):
            cnt = cnt + res[:, j * LANES:(j + 1) * LANES]
        rb[rows, :] = res.astype(jnp.bfloat16)
        return cnt

    def m_chunk(t, q, first):
        m, r, sc = scale_of(t, q)
        with jax.named_scope("mchunk"):
            for b in range(nkb):
                rows = slice(b * KB, (b + 1) * KB)
                cnt = m_rows(q, rows, KB, sc)
                n_acc[rows, :] = jnp.where(first, cnt, n_acc[rows, :] + cnt)
            s = jnp.dot(rb[...], xg[q], preferred_element_type=jnp.float32)
            s_acc[...] = jnp.where(first, s, s_acc[...] + s)
        return m, r

    order = (0, 1, 3, 2) if nx == 4 else tuple(range(nx))
    for off in order:
        q = lax.rem(xi + off, nx)
        n_in = (fits - 1) if off == 0 else fits
        part = xg.at[q, pl.ds(0, n_in * n_rows)]
        with jax.named_scope("xwait"):
            pltpu.make_async_copy(part, part, x_recv.at[q]).wait()
        e_dot(q)
        with jax.named_scope("esoft"):
            e_soft(0, q)
        stat_start(0, q)

    def sweep(t, carry):
        def m_body(q, c):
            stat_wait(t, q, False)
            m_chunk(t, q, q == 0)
            return c

        lax.fori_loop(0, nx, m_body, 0)

        with jax.named_scope("terms"):
            for b in range(nkb):
                rows = slice(b * KB, (b + 1) * KB)
                cnt = jnp.sum(n_acc[rows, :], axis=1, keepdims=True)
                mu = s_acc[rows, :] / (cnt + EPS_COUNT)
                logw = jnp.log((cnt + PRIOR_ALPHA) / (total_pts + total_comp * PRIOR_ALPHA))
                comp_terms(t + 1, rows, mu, logw)
        e_dot(0)

        def e_body(q, c):
            e_dot(q + 1)
            with jax.named_scope("esoft"):
                e_soft(t + 1, q)
            with jax.named_scope("stsend"):
                stat_start(t + 1, q)
            return c

        lax.fori_loop(0, nx - 1, e_body, 0)
        with jax.named_scope("esoft"):
            e_soft(t + 1, nx - 1)
        with jax.named_scope("stsend"):
            stat_start(t + 1, nx - 1)
        return carry

    lax.fori_loop(0, sweeps - 1, sweep, 0)

    tl = sweeps - 1

    sq_rows = []
    for j in range(lb):
        xb = xg[xi, j * LANES:(j + 1) * LANES, :].astype(jnp.float32)
        sq_rows.append(jnp.sum(jnp.transpose(xb * xb), axis=0, keepdims=True))
    sq = jnp.concatenate(sq_rows, axis=0)

    def m_last(q, c):
        stat_wait(tl, q, False)
        m, r = m_chunk(tl, q, q == 0)
        return c

    lax.fori_loop(0, nx, m_last, 0)
    m, r, _ = scale_of(tl, xi)
    small_src[1, 0:lb, :] = m * LN2 + jnp.log(r) - beta_ref[tl] * sq

    right = lax.rem(xi + 1, nx)
    left = lax.rem(xi + nx - 1, nx)
    far = lax.rem(xi + 2, nx)
    sib = xi * fits + lax.rem(fit + 1, fits)

    def span(x, p):
        return pl.ds(pl.multiple_of(x * kd + p * kp, kp), kp)

    def mu_copy(x, p, send_sem, recv_sem, r):
        part = mu_all.at[fit, span(x, p)]
        return pltpu.make_async_remote_copy(src_ref=part, dst_ref=part, send_sem=send_sem, recv_sem=recv_sem,
                                            device_id=dev(comp, r), device_id_type=MESH)

    waits = []
    half_p = pieces // 2
    porder = [p // 2 + (p % 2) * half_p for p in range(pieces)]
    for p in porder:
        for b in range(kp // LANES):
            rows = pl.ds(p * kp + b * LANES, LANES)
            na = n_acc[rows, :]
            cnt = jnp.sum(na, axis=1, keepdims=True)
            mu_all[fit, pl.ds(pl.multiple_of(xi * kd + p * kp + b * LANES, LANES), LANES), :] = s_acc[rows, :] / (cnt + EPS_COUNT)
            n_row_v = jnp.sum(jnp.transpose(na), axis=0, keepdims=True)
            j = p * (kp // LANES) + b
            small_src[0, j:j + 1, :] = jnp.log((n_row_v + PRIOR_ALPHA) / (total_pts + total_comp * PRIOR_ALPHA))
        to_r = mu_copy(xi, p, ag_send.at[0, p], ag_recv.at[0, p], right * fits + fit)
        to_l = mu_copy(xi, p, ag_send.at[1, p], ag_recv.at[1, p], left * fits + fit)
        to_s = mu_copy(xi, p, sib_send.at[0, p], sib_recv.at[0, p], sib)
        to_r.start()
        to_l.start()
        to_s.start()
        waits += [to_r.wait_send, to_l.wait_send, to_s.wait_send]

    sm_me = small_buf.at[row]
    sm_copies = []
    for k in range(1, n_row):
        r = lax.rem(row + k, n_row)
        cpy = pltpu.make_async_remote_copy(src_ref=small_src, dst_ref=sm_me, send_sem=sm_send, recv_sem=sm_recv,
                                           device_id=dev(comp, r), device_id_type=MESH)
        cpy.start()
        sm_copies.append(cpy)
    small_buf[row] = small_src[...]

    for i, p in enumerate(porder):
        for side, src in ((0, left), (1, right)):
            mu_copy(src, p, ag_send.at[2, p], ag_recv.at[side, p], sib).wait_recv()
            if (p < half_p) == (side == 0):
                fw = mu_copy(src, p, ag_send.at[2, p], ag_recv.at[2, p],
                             (right if side == 0 else left) * fits + fit)
                fw.start()
                waits.append(fw.wait_send)
            d = 1 if side == 0 else 3
            ts = mu_copy(src, p, sib_send.at[d, p], sib_recv.at[d, p], sib)
            ts.start()
            waits.append(ts.wait_send)
    for p in porder:
        mu_copy(far, p, ag_send.at[2, p], ag_recv.at[2, p], sib).wait_recv()
        ts = mu_copy(far, p, sib_send.at[2, p], sib_recv.at[2, p], sib)
        ts.start()
        waits.append(ts.wait_send)
    ofit = lax.rem(fit + 1, fits)
    for d, src in ((0, xi), (1, left), (3, right), (2, far)):
        for p in porder:
            part = mu_all.at[ofit, span(src, p)]
            pltpu.make_async_copy(part, part, sib_recv.at[d, p]).wait()

    part = small_buf.at[pl.ds(0, n_row - 1)]
    pltpu.make_async_copy(part, part, sm_recv).wait()
    pltpu.make_async_copy(part, part, sm_send).wait()
    for w in waits:
        w()
    def drain(t, c):
        for q in range(nx):
            stat_wait(t, q, True)
        return c
    lax.fori_loop(0, sweeps, drain, 0)
    for cpy in x_copies:
        cpy.wait_send()


def finish_kernel(fits, mu_all, small, o_mu, o_logpi, o_lse, sem):
    cp = pltpu.make_async_copy(mu_all, o_mu, sem)
    cp.start()
    row = lax.axis_index("row")
    fit = lax.rem(row, fits)
    first = row - fit
    n_row, _, srows, _ = small.shape
    nx = n_row // fits
    kd = o_logpi.shape[1] // nx
    n_rows = o_lse.shape[1]
    per = n_rows // LANES
    for f in range(fits):
        for x in range(nx):
            for j in range(kd // LANES):
                o_logpi[f:f + 1, x * kd + j * LANES:x * kd + (j + 1) * LANES] = small[x * fits + f, 0, j:j + 1, :]
        for j in range(per):
            v = small[first + f, 1, j:j + 1, :]
            for g in range(1, fits):
                v = jnp.where(fit == g, small[first + f, 1, g * per + j:g * per + j + 1, :], v)
            o_lse[f:f + 1, j * LANES:(j + 1) * LANES] = v
    cp.wait()


def solution(mesh):
    comp_size = mesh.shape["comp"]
    row_size = mesh.shape["row"]

    def local_fit(x_local, mu_init, logpi_init, inv_temp):
        n_rows, full_dim = x_local.shape
        fits, n_local, half = mu_init.shape
        sweeps = inv_temp.shape[0]
        nx = row_size // fits
        kd = n_local // nx
        cp = n_rows * fits
        n_peer = comp_size * nx
        pieces = 4
        dims = {"fits": fits, "comp": comp_size, "row": row_size, "sweeps": sweeps, "pieces": pieces}
        f32, bf16 = jnp.float32, jnp.bfloat16
        dma = pltpu.SemaphoreType.DMA
        srows = cp // LANES
        hbm = pl.BlockSpec(memory_space=pltpu.HBM)
        vmem = pl.BlockSpec(memory_space=pltpu.VMEM)
        mu, small = pl.pallas_call(
            functools.partial(em_kernel, dims),
            out_shape=(pltpu.VMEM((fits, n_local, half), f32),
                       pltpu.VMEM((row_size, 2, kd // LANES, LANES), f32)),
            in_specs=[hbm] * 4,
            out_specs=(vmem, vmem),
            scratch_shapes=[
                pltpu.SMEM((sweeps,), f32),
                pltpu.VMEM((n_rows, full_dim), bf16),
                pltpu.VMEM((fits, n_local), f32),
                pltpu.VMEM((nx, cp, half), bf16),
                pltpu.VMEM((kd, half), f32),
                pltpu.VMEM((kd, half), bf16),
                pltpu.VMEM((kd, LANES), f32),
                pltpu.VMEM((nx, kd, cp), f32),
                pltpu.VMEM((kd, cp), bf16),
                pltpu.VMEM((kd, half), f32),
                pltpu.VMEM((kd, LANES), f32),
                pltpu.VMEM((sweeps, nx, 2, srows, LANES), f32),
                pltpu.VMEM((sweeps, nx, n_peer, 2, srows, LANES), f32),
                pltpu.VMEM((2, kd // LANES, LANES), f32),
                dma((4,)), dma, dma((nx,)),
                dma((sweeps, nx)), dma((sweeps, nx)),
                dma, dma,
                dma((3, pieces)), dma((3, pieces)), dma((4, pieces)), dma((4, pieces)),
            ],
            compiler_params=pltpu.CompilerParams(collective_id=0, has_side_effects=True,
                                                 vmem_limit_bytes=48 * 1024 * 1024),
        )(*[pltpu.with_memory_space_constraint(v, pltpu.HBM) for v in (inv_temp, x_local, mu_init, logpi_init)])
        return pl.pallas_call(
            functools.partial(finish_kernel, fits),
            out_shape=(jax.ShapeDtypeStruct((fits, n_local, half), f32),
                       jax.ShapeDtypeStruct((fits, n_local), f32),
                       jax.ShapeDtypeStruct((fits, n_rows), f32)),
            in_specs=[pl.BlockSpec(memory_space=pl.ANY), vmem],
            out_specs=(hbm, vmem, vmem),
            scratch_shapes=[dma],
            compiler_params=pltpu.CompilerParams(vmem_limit_bytes=8 * 1024 * 1024),
        )(pltpu.with_memory_space_constraint(mu, pltpu.VMEM), pltpu.with_memory_space_constraint(small, pltpu.VMEM))

    return jax.shard_map(
        local_fit,
        mesh=mesh,
        in_specs=(P(("grp", "row"), None), P(None, ("grp", "comp"), None), P(None, ("grp", "comp")), P()),
        out_specs=(P(None, ("grp", "comp"), None), P(None, ("grp", "comp")), P(None, ("grp", "row"))),
        check_vma=False,
    )
```

```python
import functools
import math

import jax
import jax.numpy as jnp
from jax import lax
from jax.experimental import pallas as pl
from jax.experimental.pallas import tpu as pltpu
from jax.sharding import PartitionSpec as P

EPS_COUNT = 1e-6
PRIOR_ALPHA = 1e-3
LOG2E = math.log2(math.e)
LN2 = math.log(2.0)
LANES = 128
MESH = pl.DeviceIdType.MESH
NT = (((1,), (1,)), ((), ()))


def em_kernel(dims, beta_hbm, x_hbm, mu_hbm, logpi_hbm, mu_all, small_buf,
              beta_ref, x_ref, logpi_ref, xg, mu_f, mu_b, a_bc, lbuf, rb, s_acc, n_acc,
              stat_src, stat_buf, small_src, a_row, xm_b, xa_row, xa_bc, xbuf, xrb, xs_acc, xn_acc,
              loc_sem, x_send, x_recv, st_send, st_recv, sm_send, sm_recv,
              bk_send, bk_recv, ar_send, ar_recv, far_send, far_recv, sib_send, sib_recv):
    fits, n_comp, n_row, sweeps = dims["fits"], dims["comp"], dims["row"], dims["sweeps"]
    n_rows, half = x_ref.shape[0], mu_f.shape[1]
    nx = n_row // fits
    kd = mu_f.shape[0]
    cp = n_rows * fits
    lb = cp // LANES
    n_peer = n_comp * nx
    total_pts = n_rows * n_row
    total_comp = kd * nx * n_comp

    grp = lax.axis_index("grp")
    comp = lax.axis_index("comp")
    row = lax.axis_index("row")
    fit = lax.rem(row, fits)
    xi = row // fits
    me = comp * nx + xi

    def dev(c, r):
        return (grp, c, r)

    def stat_peer(k):
        d_c, d_x = k // nx, k % nx
        return lax.rem(comp + d_c, n_comp), lax.rem(xi + d_x, nx)

    barrier = pltpu.get_barrier_semaphore()
    n_sig = 0
    for k in range(1, n_peer):
        c, x = stat_peer(k)
        pl.semaphore_signal(barrier, inc=1, device_id=dev(c, x * fits + fit), device_id_type=MESH)
        n_sig += 1
    for k in range(nx):
        for f in range(1, fits):
            x = lax.rem(xi + k, nx)
            pl.semaphore_signal(barrier, inc=1, device_id=dev(comp, x * fits + lax.rem(fit + f, fits)), device_id_type=MESH)
            n_sig += 1

    loads = [pltpu.make_async_copy(x_hbm, x_ref, loc_sem.at[0]),
             pltpu.make_async_copy(mu_hbm.at[fit, pl.ds(pl.multiple_of(xi * kd, kd), kd), :], mu_f, loc_sem.at[1]),
             pltpu.make_async_copy(logpi_hbm, logpi_ref, loc_sem.at[2]),
             pltpu.make_async_copy(beta_hbm, beta_ref, loc_sem.at[3])]
    for cpy in loads:
        cpy.start()

    def comp_terms(t, rows, mu, logw):
        beta = beta_ref[t]
        sq = jnp.sum(mu * mu, axis=1, keepdims=True)
        a = (logw - beta * sq) * LOG2E
        a_bc[rows, :] = jnp.broadcast_to(a, (a.shape[0], LANES))
        mu_b[rows, :] = mu.astype(jnp.bfloat16)

    for cpy in loads:
        cpy.wait()
    for b in range(kd // LANES):
        rows = pl.ds(b * LANES, LANES)
        lw = logpi_ref[:, pl.ds(pl.multiple_of(xi * kd + b * LANES, LANES), LANES)]
        pick = lax.broadcasted_iota(jnp.int32, (fits, LANES), 0) == fit
        lw = jnp.sum(jnp.where(pick, lw, 0.0), axis=0, keepdims=True)
        lw = jnp.transpose(jnp.broadcast_to(lw, (LANES, LANES)))
        comp_terms(0, rows, mu_f[rows, :], lw[:, 0:1])

    with jax.named_scope("bar"):
        pl.semaphore_wait(barrier, n_sig)

    def x_cols(f):
        return pl.ds(pl.multiple_of(f * half, half), half)

    my_rows = pl.ds(pl.multiple_of(fit * n_rows, n_rows), n_rows)
    x_copies = []
    for k in (0, 1, 3, 2) if nx == 4 else range(nx):
        for f in range(fits):
            if k == 0 and f == 0:
                continue
            x = lax.rem(xi + k, nx)
            ft = lax.rem(fit + f, fits)
            cpy = pltpu.make_async_remote_copy(
                src_ref=x_ref.at[:, x_cols(ft)],
                dst_ref=xg.at[xi, my_rows],
                send_sem=x_send, recv_sem=x_recv.at[xi],
                device_id=dev(comp, x * fits + ft), device_id_type=MESH)
            cpy.start()
            x_copies.append(cpy)
    xg[xi, my_rows, :] = x_ref[:, x_cols(fit)]

    def lanes_tile(v):
        return jnp.concatenate([v] * lb, axis=1)

    KB = 128
    nkb = kd // KB

    def e_dot(q):
        with jax.named_scope("edot"):
            lbuf[q] = lax.dot_general(mu_b[...], xg[q], NT, preferred_element_type=jnp.float32)

    def e_soft(t, q):
        c2 = beta_ref[t] * (2.0 * LOG2E)
        m8 = jnp.full((8, cp), -jnp.inf, jnp.float32)
        for b in range(nkb):
            rows = slice(b * KB, (b + 1) * KB)
            l = lbuf[q, rows, :] * c2 + lanes_tile(a_bc[rows, :])
            lbuf[q, rows, :] = l
            m8 = jnp.maximum(m8, jnp.max(l.reshape(KB // 8, 8, cp), axis=0))
        m = jnp.max(m8, axis=0, keepdims=True)
        r8 = jnp.zeros((8, cp), jnp.float32)
        for b in range(nkb):
            rows = slice(b * KB, (b + 1) * KB)
            p = jnp.exp2(lbuf[q, rows, :] - m)
            lbuf[q, rows, :] = p
            r8 = r8 + jnp.sum(p.reshape(KB // 8, 8, cp), axis=0)
        r = jnp.sum(r8, axis=0, keepdims=True)
        for j in range(lb):
            cols = slice(j * LANES, (j + 1) * LANES)
            for ref in (stat_src.at[t, q], stat_buf.at[t, q, me]):
                ref[0, j:j + 1, :] = m[:, cols]
                ref[1, j:j + 1, :] = r[:, cols]

    def stat_copy(t, q, k):
        c, x = stat_peer(k)
        return pltpu.make_async_remote_copy(
            src_ref=stat_src.at[t, q], dst_ref=stat_buf.at[t, q, me],
            send_sem=st_send.at[t, q], recv_sem=st_recv.at[t, q],
            device_id=dev(c, x * fits + fit), device_id_type=MESH)

    def stat_start(t, q):
        for k in range(1, n_peer):
            stat_copy(t, q, k).start()

    def stat_wait(t, q, send):
        part = stat_buf.at[t, q, pl.ds(0, n_peer - 1)]
        d = pltpu.make_async_copy(part, part, st_send.at[t, q] if send else st_recv.at[t, q])
        with jax.named_scope("stwait"):
            d.wait()

    def totals_of(t, q):
        m_all = stat_buf[t, q, :, 0]
        r_all = stat_buf[t, q, :, 1]
        m = jnp.max(m_all, axis=0)
        r = jnp.sum(r_all * jnp.exp2(m_all - m), axis=0)
        return m, r

    def scale_of(t, q):
        m, r = totals_of(t, q)
        return m, r, jnp.exp2(stat_src[t, q, 0] - m) / r

    def lane_rows(v, nrow):
        return jnp.concatenate([jnp.broadcast_to(v[j:j + 1, :], (nrow, LANES)) for j in range(lb)], axis=1)

    def m_rows(q, rows, nrow, sc):
        sc_row = jnp.concatenate([jnp.broadcast_to(sc[j:j + 1, :], (nrow, LANES)) for j in range(lb)], axis=1)
        res = lbuf[q, rows, :] * sc_row
        cnt = res[:, 0:LANES]
        for j in range(1, lb):
            cnt = cnt + res[:, j * LANES:(j + 1) * LANES]
        rb[rows, :] = res.astype(jnp.bfloat16)
        return cnt

    def m_chunk(t, q, first):
        m, r, sc = scale_of(t, q)
        with jax.named_scope("mchunk"):
            for b in range(nkb):
                rows = slice(b * KB, (b + 1) * KB)
                cnt = m_rows(q, rows, KB, sc)
                n_acc[rows, :] = jnp.where(first, cnt, n_acc[rows, :] + cnt)
            s = jnp.dot(rb[...], xg[q], preferred_element_type=jnp.float32)
            s_acc[...] = jnp.where(first, s, s_acc[...] + s)
        return m, r

    order = (0, 1, 3, 2) if nx == 4 else tuple(range(nx))
    for off in order:
        q = lax.rem(xi + off, nx)
        n_in = (fits - 1) if off == 0 else fits
        part = xg.at[q, pl.ds(0, n_in * n_rows)]
        with jax.named_scope("xwait"):
            pltpu.make_async_copy(part, part, x_recv.at[q]).wait()
        e_dot(q)
        with jax.named_scope("esoft"):
            e_soft(0, q)
        stat_start(0, q)

    right = lax.rem(xi + 1, nx)
    left = lax.rem(xi + nx - 1, nx)
    far = lax.rem(xi + 2, nx)
    sides = ((0, right), (1, left))

    def bulk_piece(p, width):
        for d, x in sides:
            rows = pl.ds(p * KB, width * KB)
            pltpu.make_async_remote_copy(
                src_ref=mu_b.at[rows], dst_ref=xm_b.at[d, rows],
                send_sem=bk_send.at[d], recv_sem=bk_recv.at[d],
                device_id=dev(comp, x * fits + fit), device_id_type=MESH).start()

    def a_copy(d, x):
        return pltpu.make_async_remote_copy(
            src_ref=a_row, dst_ref=xa_row.at[d], send_sem=ar_send.at[d], recv_sem=ar_recv.at[d],
            device_id=dev(comp, x * fits + fit), device_id_type=MESH)

    def sweep(t, last):
        def m_body(q, c):
            stat_wait(t, q, False)
            m_chunk(t, q, q == 0)
            return c

        lax.fori_loop(0, nx, m_body, 0)
        with jax.named_scope("terms"):
            for b in range(nkb):
                rows = slice(b * KB, (b + 1) * KB)
                cnt = jnp.sum(n_acc[rows, :], axis=1, keepdims=True)
                mu = s_acc[rows, :] / (cnt + EPS_COUNT)
                logw = jnp.log((cnt + PRIOR_ALPHA) / (total_pts + total_comp * PRIOR_ALPHA))
                comp_terms(t + 1, rows, mu, logw)
                if last:
                    a_row[b:b + 1, :] = jnp.transpose(a_bc[rows, :])[0:1, :]
        e_dot(0)
        if last:
            bulk_piece(0, 2)
            for d, x in sides:
                a_copy(d, x).start()

        def e_body(q, c):
            e_dot(q + 1)
            with jax.named_scope("esoft"):
                e_soft(t + 1, q)
            with jax.named_scope("stsend"):
                stat_start(t + 1, q)
                if last:
                    bulk_piece(q + 2, 1)
            return c

        lax.fori_loop(0, nx - 1, e_body, 0)
        with jax.named_scope("esoft"):
            e_soft(t + 1, nx - 1)
        with jax.named_scope("stsend"):
            stat_start(t + 1, nx - 1)
            if last:
                bulk_piece(nx + 1, nkb - nx - 1)

    def sweep_body(t, c):
        sweep(t, False)
        return c

    lax.fori_loop(0, sweeps - 2, sweep_body, 0)
    sweep(sweeps - 2, True)

    tl = sweeps - 1

    sq_rows = []
    for j in range(lb):
        xb = xg[xi, j * LANES:(j + 1) * LANES, :].astype(jnp.float32)
        sq_rows.append(jnp.sum(jnp.transpose(xb * xb), axis=0, keepdims=True))
    sq = jnp.concatenate(sq_rows, axis=0)

    kh = kd // 2
    nh = kh // KB
    c2_last = beta_ref[tl] * (2.0 * LOG2E)
    sib = xi * fits + lax.rem(fit + 1, fits)
    with jax.named_scope("bulkwait"):
        for d in range(2):
            pltpu.make_async_copy(xm_b.at[d], xm_b.at[d], bk_recv.at[d]).wait()
            pltpu.make_async_copy(xa_row.at[d], xa_row.at[d], ar_recv.at[d]).wait()
    with jax.named_scope("xterms"):
        for d in range(2):
            for b in range(nkb):
                xa_bc[d, b * KB:(b + 1) * KB, :] = jnp.transpose(jnp.broadcast_to(xa_row[d, b:b + 1, :], (KB, LANES)))

    owner = (comp * nx + left, comp * nx + right)

    def x_units(q, first, halves):
        m, r = totals_of(tl, q)
        for d, h in enumerate(halves):
            hrows = slice(h * kh, (h + 1) * kh)
            xbuf[d] = lax.dot_general(xm_b[d, hrows, :], xg[q], NT, preferred_element_type=jnp.float32)
        for d, h in enumerate(halves):
            m_j = stat_buf[tl, q, owner[d], 0]
            m_row = lane_rows(m_j, KB)
            sc_row = lane_rows(jnp.exp2(m_j - m) / r, KB)
            for b in range(nh):
                rows = slice(b * KB, (b + 1) * KB)
                grows = slice(h * kh + b * KB, h * kh + (b + 1) * KB)
                l = xbuf[d, rows, :] * c2_last + lanes_tile(xa_bc[d, grows, :])
                res = jnp.exp2(l - m_row) * sc_row
                cnt = res[:, 0:LANES]
                for j in range(1, lb):
                    cnt = cnt + res[:, j * LANES:(j + 1) * LANES]
                xrb[d, rows, :] = res.astype(jnp.bfloat16)
                xn_acc[d, rows, :] = jnp.where(first, cnt, xn_acc[d, rows, :] + cnt)
        for d, h in enumerate(halves):
            s = jnp.dot(xrb[d], xg[q], preferred_element_type=jnp.float32)
            xs_acc[d] = jnp.where(first, s, xs_acc[d] + s)

    def mean_rows(na, sa):
        return sa / (jnp.sum(na, axis=1, keepdims=True) + EPS_COUNT)

    def span(x, start, size):
        return pl.ds(pl.multiple_of(x * kd + start, KB), size)

    waits = []

    def push(x, start, size, send_sem, recv_sem, r):
        part = mu_all.at[fit, span(x, start, size)]
        cpy = pltpu.make_async_remote_copy(src_ref=part, dst_ref=part, send_sem=send_sem, recv_sem=recv_sem,
                                           device_id=dev(comp, r), device_id_type=MESH)
        cpy.start()
        waits.append(cpy.wait_send)

    def x_finish(d, h, b):
        x = (left, right)[d]
        rows = slice(b * KB, (b + 1) * KB)
        mu_all[fit, span(x, h * kh + b * KB, KB), :] = mean_rows(xn_acc[d, rows, :], xs_acc[d, rows, :])

    def xa_body(q, c):
        stat_wait(tl, q, False)
        with jax.named_scope("xunitA"):
            x_units(q, q == 0, (0, 1))
        return c

    lax.fori_loop(0, nx, xa_body, 0)
    with jax.named_scope("xfinA"):
        for b in range(nh):
            for d, x in sides:
                x_finish(d, d, b)
                push((left, right)[d], d * kh + b * KB, KB, far_send.at[d, b], far_recv.at[d, b], x * fits + fit)
        for d in range(2):
            push((left, right)[d], d * kh, kh, sib_send.at[d], sib_recv.at[d], sib)

    def m_last(q, c):
        m_chunk(tl, q, q == 0)
        return c

    lax.fori_loop(0, nx, m_last, 0)
    with jax.named_scope("ownfin"):
        m, r, _ = scale_of(tl, xi)
        small_src[1, 0:lb, :] = m * LN2 + jnp.log(r) - beta_ref[tl] * sq
        for b in range(nkb):
            rows = slice(b * KB, (b + 1) * KB)
            na = n_acc[rows, :]
            mu_all[fit, span(xi, b * KB, KB), :] = mean_rows(na, s_acc[rows, :])
            n_row_v = jnp.sum(jnp.transpose(na), axis=0, keepdims=True)
            small_src[0, b:b + 1, :] = jnp.log((n_row_v + PRIOR_ALPHA) / (total_pts + total_comp * PRIOR_ALPHA))
        push(xi, 0, kd, sib_send.at[2], sib_recv.at[2], sib)
        for k in range(1, n_row):
            r = lax.rem(row + k, n_row)
            cpy = pltpu.make_async_remote_copy(src_ref=small_src, dst_ref=small_buf.at[row], send_sem=sm_send, recv_sem=sm_recv,
                                               device_id=dev(comp, r), device_id_type=MESH)
            cpy.start()
        small_buf[row] = small_src[...]

    def xb_body(q, c):
        with jax.named_scope("xunitB"):
            x_units(q, q == 0, (1, 0))
        return c

    lax.fori_loop(0, nx, xb_body, 0)
    with jax.named_scope("xfinB"):
        for d in range(2):
            for b in range(nh):
                x_finish(d, 1 - d, b)
            push((left, right)[d], (1 - d) * kh, kh, sib_send.at[3 + d], sib_recv.at[3 + d], sib)

    with jax.named_scope("farwait"):
        for b in range(nh):
            for d in range(2):
                part = mu_all.at[fit, span(far, d * kh + b * KB, KB)]
                pltpu.make_async_copy(part, part, far_recv.at[d, b]).wait()
                k = 5 + d * nh + b
                push(far, d * kh + b * KB, KB, sib_send.at[k], sib_recv.at[k], sib)
    ofit = lax.rem(fit + 1, fits)

    def sib_wait(x, start, size, k):
        part = mu_all.at[ofit, span(x, start, size)]
        pltpu.make_async_copy(part, part, sib_recv.at[k]).wait()

    with jax.named_scope("sibwait"):
        sib_wait(xi, 0, kd, 2)
        for d, x in ((0, left), (1, right)):
            sib_wait(x, d * kh, kh, d)
            sib_wait(x, (1 - d) * kh, kh, 3 + d)
            for b in range(nh):
                sib_wait(far, d * kh + b * KB, KB, 5 + d * nh + b)

    part = small_buf.at[pl.ds(0, n_row - 1)]
    pltpu.make_async_copy(part, part, sm_recv).wait()
    pltpu.make_async_copy(part, part, sm_send).wait()
    for w in waits:
        w()
    def drain(t, c):
        for q in range(nx):
            stat_wait(t, q, True)
        return c
    lax.fori_loop(0, sweeps, drain, 0)
    for cpy in x_copies:
        cpy.wait_send()
    for d in range(2):
        pltpu.make_async_copy(xm_b.at[d], xm_b.at[d], bk_send.at[d]).wait()
        pltpu.make_async_copy(xa_row.at[d], xa_row.at[d], ar_send.at[d]).wait()


def finish_kernel(fits, mu_all, small, o_mu, o_logpi, o_lse, sem):
    cp = pltpu.make_async_copy(mu_all, o_mu, sem)
    cp.start()
    row = lax.axis_index("row")
    fit = lax.rem(row, fits)
    first = row - fit
    n_row, _, srows, _ = small.shape
    nx = n_row // fits
    kd = o_logpi.shape[1] // nx
    n_rows = o_lse.shape[1]
    per = n_rows // LANES
    for f in range(fits):
        for x in range(nx):
            for j in range(kd // LANES):
                o_logpi[f:f + 1, x * kd + j * LANES:x * kd + (j + 1) * LANES] = small[x * fits + f, 0, j:j + 1, :]
        for j in range(per):
            v = small[first + f, 1, j:j + 1, :]
            for g in range(1, fits):
                v = jnp.where(fit == g, small[first + f, 1, g * per + j:g * per + j + 1, :], v)
            o_lse[f:f + 1, j * LANES:(j + 1) * LANES] = v
    cp.wait()


def solution(mesh):
    comp_size = mesh.shape["comp"]
    row_size = mesh.shape["row"]

    def local_fit(x_local, mu_init, logpi_init, inv_temp):
        n_rows, full_dim = x_local.shape
        fits, n_local, half = mu_init.shape
        sweeps = inv_temp.shape[0]
        nx = row_size // fits
        kd = n_local // nx
        cp = n_rows * fits
        n_peer = comp_size * nx
        kb = LANES
        nh = kd // 2 // kb
        dims = {"fits": fits, "comp": comp_size, "row": row_size, "sweeps": sweeps}
        f32, bf16 = jnp.float32, jnp.bfloat16
        dma = pltpu.SemaphoreType.DMA
        srows = cp // LANES
        hbm = pl.BlockSpec(memory_space=pltpu.HBM)
        vmem = pl.BlockSpec(memory_space=pltpu.VMEM)
        mu, small = pl.pallas_call(
            functools.partial(em_kernel, dims),
            out_shape=(pltpu.VMEM((fits, n_local, half), f32),
                       pltpu.VMEM((row_size, 2, kd // LANES, LANES), f32)),
            in_specs=[hbm] * 4,
            out_specs=(vmem, vmem),
            scratch_shapes=[
                pltpu.SMEM((sweeps,), f32),
                pltpu.VMEM((n_rows, full_dim), bf16),
                pltpu.VMEM((fits, n_local), f32),
                pltpu.VMEM((nx, cp, half), bf16),
                pltpu.VMEM((kd, half), f32),
                pltpu.VMEM((kd, half), bf16),
                pltpu.VMEM((kd, LANES), f32),
                pltpu.VMEM((nx, kd, cp), f32),
                pltpu.VMEM((kd, cp), bf16),
                pltpu.VMEM((kd, half), f32),
                pltpu.VMEM((kd, LANES), f32),
                pltpu.VMEM((sweeps, nx, 2, srows, LANES), f32),
                pltpu.VMEM((sweeps, nx, n_peer, 2, srows, LANES), f32),
                pltpu.VMEM((2, kd // LANES, LANES), f32),
                pltpu.VMEM((kd // LANES, LANES), f32),
                pltpu.VMEM((2, kd, half), bf16),
                pltpu.VMEM((2, kd // LANES, LANES), f32),
                pltpu.VMEM((2, kd, LANES), f32),
                pltpu.VMEM((2, kd // 2, cp), f32),
                pltpu.VMEM((2, kd // 2, cp), bf16),
                pltpu.VMEM((2, kd // 2, half), f32),
                pltpu.VMEM((2, kd // 2, LANES), f32),
                dma((4,)), dma, dma((nx,)),
                dma((sweeps, nx)), dma((sweeps, nx)),
                dma, dma,
                dma((2,)), dma((2,)), dma((2,)), dma((2,)),
                dma((2, nh)), dma((2, nh)), dma((5 + 2 * nh,)), dma((5 + 2 * nh,)),
            ],
            compiler_params=pltpu.CompilerParams(collective_id=0, has_side_effects=True,
                                                 vmem_limit_bytes=48 * 1024 * 1024),
        )(*[pltpu.with_memory_space_constraint(v, pltpu.HBM) for v in (inv_temp, x_local, mu_init, logpi_init)])
        return pl.pallas_call(
            functools.partial(finish_kernel, fits),
            out_shape=(jax.ShapeDtypeStruct((fits, n_local, half), f32),
                       jax.ShapeDtypeStruct((fits, n_local), f32),
                       jax.ShapeDtypeStruct((fits, n_rows), f32)),
            in_specs=[pl.BlockSpec(memory_space=pl.ANY), vmem],
            out_specs=(hbm, vmem, vmem),
            scratch_shapes=[dma],
            compiler_params=pltpu.CompilerParams(vmem_limit_bytes=8 * 1024 * 1024),
        )(pltpu.with_memory_space_constraint(mu, pltpu.VMEM), pltpu.with_memory_space_constraint(small, pltpu.VMEM))

    return jax.shard_map(
        local_fit,
        mesh=mesh,
        in_specs=(P(("grp", "row"), None), P(None, ("grp", "comp"), None), P(None, ("grp", "comp")), P()),
        out_specs=(P(None, ("grp", "comp"), None), P(None, ("grp", "comp")), P(None, ("grp", "row"))),
        check_vma=False,
    )
```

```python
import functools
import math

import jax
import jax.numpy as jnp
from jax import lax
from jax.experimental import pallas as pl
from jax.experimental.pallas import tpu as pltpu
from jax.sharding import PartitionSpec as P

EPS_COUNT = 1e-6
PRIOR_ALPHA = 1e-3
LOG2E = math.log2(math.e)
LN2 = math.log(2.0)
LANES = 128
MESH = pl.DeviceIdType.MESH
NT = (((1,), (1,)), ((), ()))


def em_kernel(dims, beta_hbm, x_hbm, mu_hbm, logpi_hbm, mu_all, small_buf,
              beta_ref, x_ref, logpi_ref, xg, mu_f, mu_b, a_bc, lbuf, rb, s_acc, n_acc,
              stat_src, stat_buf, small_src, a_row, xm_b, xa_row, xa_bc, xbuf_a, xbuf_b, xrb, xs_acc, xn_acc,
              loc_sem, x_send, x_recv, st_send, st_recv, sm_send, sm_recv,
              bk_send, bk_recv, ar_send, ar_recv, far_send, far_recv, sib_send, sib_recv):
    fits, n_comp, n_row, sweeps = dims["fits"], dims["comp"], dims["row"], dims["sweeps"]
    n_rows, half = x_ref.shape[0], mu_f.shape[1]
    nx = n_row // fits
    kd = mu_f.shape[0]
    cp = n_rows * fits
    lb = cp // LANES
    n_peer = n_comp * nx
    total_pts = n_rows * n_row
    total_comp = kd * nx * n_comp

    grp = lax.axis_index("grp")
    comp = lax.axis_index("comp")
    row = lax.axis_index("row")
    fit = lax.rem(row, fits)
    xi = row // fits
    me = comp * nx + xi

    def dev(c, r):
        return (grp, c, r)

    def hops(k):
        d_c, d_x = k // nx, k % nx
        return min(d_c, n_comp - d_c) + min(d_x, nx - d_x)

    peer_order = sorted(range(1, n_peer), key=lambda k: -hops(k))
    comp_at = [lax.rem(comp + d, n_comp) for d in range(n_comp)]
    row_at = [lax.rem(xi + d, nx) * fits + fit for d in range(nx)]

    def stat_peer(k):
        return dev(comp_at[k // nx], row_at[k % nx])

    barrier = pltpu.get_barrier_semaphore()
    n_sig = 0
    for k in peer_order:
        pl.semaphore_signal(barrier, inc=1, device_id=stat_peer(k), device_id_type=MESH)
        n_sig += 1
    for k in range(nx):
        for f in range(1, fits):
            x = lax.rem(xi + k, nx)
            pl.semaphore_signal(barrier, inc=1, device_id=dev(comp, x * fits + lax.rem(fit + f, fits)), device_id_type=MESH)
            n_sig += 1

    loads = [pltpu.make_async_copy(x_hbm, x_ref, loc_sem.at[0]),
             pltpu.make_async_copy(mu_hbm.at[fit, pl.ds(pl.multiple_of(xi * kd, kd), kd), :], mu_f, loc_sem.at[1]),
             pltpu.make_async_copy(logpi_hbm, logpi_ref, loc_sem.at[2]),
             pltpu.make_async_copy(beta_hbm, beta_ref, loc_sem.at[3])]
    for cpy in loads:
        cpy.start()

    def comp_terms(t, rows, mu, logw):
        beta = beta_ref[t]
        sq = jnp.sum(mu * mu, axis=1, keepdims=True)
        a = (logw - beta * sq) * LOG2E
        a_bc[rows, :] = jnp.broadcast_to(a, (a.shape[0], LANES))
        mu_b[rows, :] = mu.astype(jnp.bfloat16)

    for cpy in loads:
        cpy.wait()
    for b in range(kd // LANES):
        rows = pl.ds(b * LANES, LANES)
        lw = logpi_ref[:, pl.ds(pl.multiple_of(xi * kd + b * LANES, LANES), LANES)]
        pick = lax.broadcasted_iota(jnp.int32, (fits, LANES), 0) == fit
        lw = jnp.sum(jnp.where(pick, lw, 0.0), axis=0, keepdims=True)
        lw = jnp.transpose(jnp.broadcast_to(lw, (LANES, LANES)))
        comp_terms(0, rows, mu_f[rows, :], lw[:, 0:1])

    with jax.named_scope("bar"):
        pl.semaphore_wait(barrier, n_sig)

    def x_cols(f):
        return pl.ds(pl.multiple_of(f * half, half), half)

    my_rows = pl.ds(pl.multiple_of(fit * n_rows, n_rows), n_rows)
    x_copies = []
    for k in (0, 1, 3, 2) if nx == 4 else range(nx):
        for f in range(fits):
            if k == 0 and f == 0:
                continue
            x = lax.rem(xi + k, nx)
            ft = lax.rem(fit + f, fits)
            cpy = pltpu.make_async_remote_copy(
                src_ref=x_ref.at[:, x_cols(ft)],
                dst_ref=xg.at[xi, my_rows],
                send_sem=x_send, recv_sem=x_recv.at[xi],
                device_id=dev(comp, x * fits + ft), device_id_type=MESH)
            cpy.start()
            x_copies.append(cpy)
    xg[xi, my_rows, :] = x_ref[:, x_cols(fit)]

    def lanes_tile(v):
        return jnp.concatenate([v] * lb, axis=1)

    KB = 128
    nkb = kd // KB

    def e_dot(q):
        with jax.named_scope("edot"):
            lbuf[q] = lax.dot_general(mu_b[...], xg[q], NT, preferred_element_type=jnp.float32)

    def e_soft(t, q):
        c2 = beta_ref[t] * (2.0 * LOG2E)
        m8 = jnp.full((8, cp), -jnp.inf, jnp.float32)
        for b in range(nkb):
            rows = slice(b * KB, (b + 1) * KB)
            l = lbuf[q, rows, :] * c2 + lanes_tile(a_bc[rows, :])
            lbuf[q, rows, :] = l
            m8 = jnp.maximum(m8, jnp.max(l.reshape(KB // 8, 8, cp), axis=0))
        m = jnp.max(m8, axis=0, keepdims=True)
        r8 = jnp.zeros((8, cp), jnp.float32)
        for b in range(nkb):
            rows = slice(b * KB, (b + 1) * KB)
            p = jnp.exp2(lbuf[q, rows, :] - m)
            lbuf[q, rows, :] = p
            r8 = r8 + jnp.sum(p.reshape(KB // 8, 8, cp), axis=0)
        r = jnp.sum(r8, axis=0, keepdims=True)
        for j in range(lb):
            cols = slice(j * LANES, (j + 1) * LANES)
            for ref in (stat_src.at[t, q], stat_buf.at[t, q, me]):
                ref[0, j:j + 1, :] = m[:, cols]
                ref[1, j:j + 1, :] = r[:, cols]

    def stat_copy(t, q, k):
        return pltpu.make_async_remote_copy(
            src_ref=stat_src.at[t, q], dst_ref=stat_buf.at[t, q, me],
            send_sem=st_send.at[t, q], recv_sem=st_recv.at[t, q],
            device_id=stat_peer(k), device_id_type=MESH)

    def stat_start(t, q):
        for k in peer_order:
            stat_copy(t, q, k).start()

    def stat_wait(t, q, send):
        part = stat_buf.at[t, q, pl.ds(0, n_peer - 1)]
        d = pltpu.make_async_copy(part, part, st_send.at[t, q] if send else st_recv.at[t, q])
        with jax.named_scope("stwait"):
            d.wait()

    def totals_of(t, q):
        m_all = stat_buf[t, q, :, 0]
        r_all = stat_buf[t, q, :, 1]
        m = jnp.max(m_all, axis=0)
        r = jnp.sum(r_all * jnp.exp2(m_all - m), axis=0)
        return m, r

    def scale_of(t, q):
        m, r = totals_of(t, q)
        return m, r, jnp.exp2(stat_src[t, q, 0] - m) / r

    def lane_rows(v, nrow):
        return jnp.concatenate([jnp.broadcast_to(v[j:j + 1, :], (nrow, LANES)) for j in range(lb)], axis=1)

    def m_rows(q, rows, nrow, sc):
        sc_row = jnp.concatenate([jnp.broadcast_to(sc[j:j + 1, :], (nrow, LANES)) for j in range(lb)], axis=1)
        res = lbuf[q, rows, :] * sc_row
        cnt = res[:, 0:LANES]
        for j in range(1, lb):
            cnt = cnt + res[:, j * LANES:(j + 1) * LANES]
        rb[rows, :] = res.astype(jnp.bfloat16)
        return cnt

    def m_chunk(t, q, first):
        m, r, sc = scale_of(t, q)
        with jax.named_scope("mchunk"):
            for b in range(nkb):
                rows = slice(b * KB, (b + 1) * KB)
                cnt = m_rows(q, rows, KB, sc)
                n_acc[rows, :] = jnp.where(first, cnt, n_acc[rows, :] + cnt)
            s = jnp.dot(rb[...], xg[q], preferred_element_type=jnp.float32)
            s_acc[...] = jnp.where(first, s, s_acc[...] + s)
        return m, r

    order = (0, 1, 3, 2) if nx == 4 else tuple(range(nx))
    for off in order:
        q = lax.rem(xi + off, nx)
        n_in = (fits - 1) if off == 0 else fits
        part = xg.at[q, pl.ds(0, n_in * n_rows)]
        with jax.named_scope("xwait"):
            pltpu.make_async_copy(part, part, x_recv.at[q]).wait()
        e_dot(q)
        with jax.named_scope("esoft"):
            e_soft(0, q)
        stat_start(0, q)

    right = lax.rem(xi + 1, nx)
    left = lax.rem(xi + nx - 1, nx)
    far = lax.rem(xi + 2, nx)
    sides = ((0, right), (1, left))

    kh = kd // 2
    nh = kh // KB

    def bulk_copy(d, x, h):
        rows = slice(h * kh, (h + 1) * kh)
        return pltpu.make_async_remote_copy(
            src_ref=mu_b.at[rows], dst_ref=xm_b.at[d, rows],
            send_sem=bk_send.at[d, h], recv_sem=bk_recv.at[d, h],
            device_id=dev(comp, x * fits + fit), device_id_type=MESH)

    def a_copy(d, x):
        return pltpu.make_async_remote_copy(
            src_ref=a_row, dst_ref=xa_row.at[d], send_sem=ar_send.at[d], recv_sem=ar_recv.at[d],
            device_id=dev(comp, x * fits + fit), device_id_type=MESH)

    def sweep(t, last):
        def m_body(q, c):
            stat_wait(t, q, False)
            m_chunk(t, q, q == 0)
            return c

        lax.fori_loop(0, nx, m_body, 0)
        with jax.named_scope("terms"):
            for b in range(nkb):
                rows = slice(b * KB, (b + 1) * KB)
                cnt = jnp.sum(n_acc[rows, :], axis=1, keepdims=True)
                mu = s_acc[rows, :] / (cnt + EPS_COUNT)
                logw = jnp.log((cnt + PRIOR_ALPHA) / (total_pts + total_comp * PRIOR_ALPHA))
                comp_terms(t + 1, rows, mu, logw)
        if last:
            for d, x in sides:
                bulk_copy(d, x, d).start()
        e_dot(0)
        if last:
            for b in range(nkb):
                a_row[b:b + 1, :] = jnp.transpose(a_bc[b * KB:(b + 1) * KB, :])[0:1, :]
            for d, x in sides:
                a_copy(d, x).start()

        def e_body(q, c):
            e_dot(q + 1)
            with jax.named_scope("esoft"):
                e_soft(t + 1, q)
            with jax.named_scope("stsend"):
                stat_start(t + 1, q)
            return c

        lax.fori_loop(0, nx - 1, e_body, 0)
        with jax.named_scope("esoft"):
            e_soft(t + 1, nx - 1)
        with jax.named_scope("stsend"):
            stat_start(t + 1, nx - 1)

    def sweep_body(t, c):
        sweep(t, False)
        return c

    lax.fori_loop(0, sweeps - 2, sweep_body, 0)
    sweep(sweeps - 2, True)

    tl = sweeps - 1

    sq_rows = []
    for j in range(lb):
        xb = xg[xi, j * LANES:(j + 1) * LANES, :].astype(jnp.float32)
        sq_rows.append(jnp.sum(jnp.transpose(xb * xb), axis=0, keepdims=True))
    sq = jnp.concatenate(sq_rows, axis=0)

    c2_last = beta_ref[tl] * (2.0 * LOG2E)
    sib = xi * fits + lax.rem(fit + 1, fits)

    for d, x in sides:
        bulk_copy(d, x, 1 - d).start()

    def x_ready(halves):
        with jax.named_scope("bulkwait"):
            for d, h in enumerate(halves):
                bulk_copy(d, left, h).wait_recv()

    def x_terms(halves):
        with jax.named_scope("xterms"):
            for d, h in enumerate(halves):
                for b in range(h * nh, (h + 1) * nh):
                    xa_bc[d, b * KB:(b + 1) * KB, :] = jnp.transpose(jnp.broadcast_to(xa_row[d, b:b + 1, :], (KB, LANES)))

    x_ready((0, 1))
    owner = (comp * nx + left, comp * nx + right)

    def x_dot(buf, q, halves):
        for d, h in enumerate(halves):
            buf[d] = lax.dot_general(xm_b[d, h * kh:(h + 1) * kh, :], xg[q], NT, preferred_element_type=jnp.float32)

    def x_scales(q):
        m, r = totals_of(tl, q)
        res = []
        for d in range(2):
            m_j = stat_buf[tl, q, owner[d], 0]
            res.append((lane_rows(m_j, KB), lane_rows(jnp.exp2(m_j - m) / r, KB)))
        return res

    def x_resp(buf, q, d, h, scales, first):
        m_row, sc_row = scales[d]
        for b in range(nh):
            rows = slice(b * KB, (b + 1) * KB)
            l = buf[d, rows, :] * c2_last + lanes_tile(xa_bc[d, h * kh + b * KB:h * kh + (b + 1) * KB, :])
            res = jnp.exp2(l - m_row) * sc_row
            cnt = res[:, 0:LANES]
            for j in range(1, lb):
                cnt = cnt + res[:, j * LANES:(j + 1) * LANES]
            xrb[q, d, rows, :] = res.astype(jnp.bfloat16)
            xn_acc[d, rows, :] = jnp.where(first, cnt, xn_acc[d, rows, :] + cnt)

    def x_sum(q, d, first):
        s = jnp.dot(xrb[q, d], xg[q], preferred_element_type=jnp.float32)
        xs_acc[d] = jnp.where(first, s, xs_acc[d] + s)

    def x_units(buf, q, first, halves):
        scales = x_scales(q)
        for d, h in enumerate(halves):
            x_resp(buf, q, d, h, scales, first)
            x_sum(q, d, first)

    def mean_rows(na, sa):
        return sa / (jnp.sum(na, axis=1, keepdims=True) + EPS_COUNT)

    def span(x, start, size):
        return pl.ds(pl.multiple_of(x * kd + start, KB), size)

    waits = []

    def push(x, start, size, send_sem, recv_sem, r):
        part = mu_all.at[fit, span(x, start, size)]
        cpy = pltpu.make_async_remote_copy(src_ref=part, dst_ref=part, send_sem=send_sem, recv_sem=recv_sem,
                                           device_id=dev(comp, r), device_id_type=MESH)
        cpy.start()
        waits.append(cpy.wait_send)

    def x_finish(d, h, b):
        x = (left, right)[d]
        rows = slice(b * KB, (b + 1) * KB)
        mu_all[fit, span(x, h * kh + b * KB, KB), :] = mean_rows(xn_acc[d, rows, :], xs_acc[d, rows, :])

    with jax.named_scope("xdotA"):
        for q in range(nx):
            x_dot(xbuf_a.at[q], q, (0, 1))
    with jax.named_scope("arwait"):
        for d in range(2):
            a_copy(d, left).wait_recv()
    x_terms((0, 1))
    x_terms((1, 0))

    def x_last(buf, q, halves, done):
        scales = x_scales(q)
        for d, h in enumerate(halves):
            x_resp(buf, q, d, h, scales, False)
            x_sum(q, d, False)
            for b in range(nh):
                x_finish(d, h, b)
            for b in range(nh):
                done(d, h, b)

    def xa_body(q, c):
        stat_wait(tl, q, False)
        with jax.named_scope("xunitA"):
            x_units(xbuf_a.at[q], q, q == 0, (0, 1))
        m_chunk(tl, q, q == 0)
        return c

    lax.fori_loop(0, nx - 2, xa_body, 0)
    stat_wait(tl, nx - 2, False)
    with jax.named_scope("xunitA"):
        x_units(xbuf_a.at[nx - 2], nx - 2, False, (0, 1))
    ql = nx - 1
    stat_wait(tl, ql, False)

    def a_done(d, h, b):
        x = (left, right)[d]
        push(x, h * kh + b * KB, KB, far_send.at[d, b], far_recv.at[d, b], sides[d][1] * fits + fit)
        if b == nh - 1:
            push(x, h * kh, kh, sib_send.at[d], sib_recv.at[d], sib)

    with jax.named_scope("xfinA"):
        x_last(xbuf_a.at[ql], ql, (0, 1), a_done)
    m_chunk(tl, nx - 2, False)
    m_chunk(tl, ql, False)
    with jax.named_scope("ownfin"):
        m, r, _ = scale_of(tl, xi)
        small_src[1, 0:lb, :] = m * LN2 + jnp.log(r) - beta_ref[tl] * sq
        for b in range(nkb):
            rows = slice(b * KB, (b + 1) * KB)
            na = n_acc[rows, :]
            mu_all[fit, span(xi, b * KB, KB), :] = mean_rows(na, s_acc[rows, :])
            n_row_v = jnp.sum(jnp.transpose(na), axis=0, keepdims=True)
            small_src[0, b:b + 1, :] = jnp.log((n_row_v + PRIOR_ALPHA) / (total_pts + total_comp * PRIOR_ALPHA))
        push(xi, 0, kd, sib_send.at[2], sib_recv.at[2], sib)
        for k in range(1, n_row):
            r = lax.rem(row + k, n_row)
            cpy = pltpu.make_async_remote_copy(src_ref=small_src, dst_ref=small_buf.at[row], send_sem=sm_send, recv_sem=sm_recv,
                                               device_id=dev(comp, r), device_id_type=MESH)
            cpy.start()
        small_buf[row] = small_src[...]

    x_ready((1, 0))
    with jax.named_scope("xunitB"):
        x_dot(xbuf_b.at[0], 0, (1, 0))
        for q in range(nx - 1):
            x_dot(xbuf_b.at[q + 1], q + 1, (1, 0))
            scales = x_scales(q)
            for d, h in enumerate((1, 0)):
                x_resp(xbuf_b.at[q], q, d, h, scales, q == 0)
            if q > 0:
                for d in range(2):
                    x_sum(q - 1, d, q == 1)
        for d in range(2):
            x_sum(nx - 2, d, False)

    def b_done(d, h, b):
        if b % 2:
            k = 3 + 2 * d + b // 2
            push((left, right)[d], h * kh + (b - 1) * KB, 2 * KB, sib_send.at[k], sib_recv.at[k], sib)

    with jax.named_scope("xfinB"):
        x_last(xbuf_b.at[ql], ql, (1, 0), b_done)

    with jax.named_scope("farwait"):
        for b in range(nh):
            for d in range(2):
                part = mu_all.at[fit, span(far, d * kh + b * KB, KB)]
                pltpu.make_async_copy(part, part, far_recv.at[d, b]).wait()
                k = 7 + d * nh + b
                push(far, d * kh + b * KB, KB, sib_send.at[k], sib_recv.at[k], sib)
    ofit = lax.rem(fit + 1, fits)

    def sib_wait(x, start, size, k):
        part = mu_all.at[ofit, span(x, start, size)]
        pltpu.make_async_copy(part, part, sib_recv.at[k]).wait()

    with jax.named_scope("sibwait"):
        sib_wait(xi, 0, kd, 2)
        for d, x in ((0, left), (1, right)):
            sib_wait(x, d * kh, kh, d)
            sib_wait(x, (1 - d) * kh, kh // 2, 3 + 2 * d)
            sib_wait(x, (1 - d) * kh + kh // 2, kh // 2, 4 + 2 * d)
            for b in range(nh):
                sib_wait(far, d * kh + b * KB, KB, 7 + d * nh + b)

    part = small_buf.at[pl.ds(0, n_row - 1)]
    pltpu.make_async_copy(part, part, sm_recv).wait()
    pltpu.make_async_copy(part, part, sm_send).wait()
    for w in waits:
        w()
    def drain(t, c):
        for q in range(nx):
            stat_wait(t, q, True)
        return c
    lax.fori_loop(0, sweeps, drain, 0)
    for cpy in x_copies:
        cpy.wait_send()
    for d in range(2):
        bulk_copy(d, left, 0).wait_send()
        bulk_copy(d, left, 1).wait_send()
        a_copy(d, left).wait_send()


def finish_kernel(fits, mu_all, small, o_mu, o_logpi, o_lse, sem):
    step = mu_all.shape[1] // 8
    for f in range(fits):
        for p in range(8):
            part = pl.ds(p * step, step)
            pltpu.make_async_copy(mu_all.at[f, part], o_mu.at[f, part], sem).start()
    row = lax.axis_index("row")
    fit = lax.rem(row, fits)
    first = row - fit
    n_row, _, srows, _ = small.shape
    nx = n_row // fits
    kd = o_logpi.shape[1] // nx
    n_rows = o_lse.shape[1]
    per = n_rows // LANES
    for f in range(fits):
        for x in range(nx):
            for j in range(kd // LANES):
                o_logpi[f:f + 1, x * kd + j * LANES:x * kd + (j + 1) * LANES] = small[x * fits + f, 0, j:j + 1, :]
        for j in range(per):
            v = small[first + f, 1, j:j + 1, :]
            for g in range(1, fits):
                v = jnp.where(fit == g, small[first + f, 1, g * per + j:g * per + j + 1, :], v)
            o_lse[f:f + 1, j * LANES:(j + 1) * LANES] = v
    pltpu.make_async_copy(mu_all, o_mu, sem).wait()


def solution(mesh):
    comp_size = mesh.shape["comp"]
    row_size = mesh.shape["row"]

    def local_fit(x_local, mu_init, logpi_init, inv_temp):
        n_rows, full_dim = x_local.shape
        fits, n_local, half = mu_init.shape
        sweeps = inv_temp.shape[0]
        nx = row_size // fits
        kd = n_local // nx
        cp = n_rows * fits
        n_peer = comp_size * nx
        kb = LANES
        nh = kd // 2 // kb
        dims = {"fits": fits, "comp": comp_size, "row": row_size, "sweeps": sweeps}
        f32, bf16 = jnp.float32, jnp.bfloat16
        dma = pltpu.SemaphoreType.DMA
        srows = cp // LANES
        hbm = pl.BlockSpec(memory_space=pltpu.HBM)
        vmem = pl.BlockSpec(memory_space=pltpu.VMEM)
        mu, small = pl.pallas_call(
            functools.partial(em_kernel, dims),
            out_shape=(pltpu.VMEM((fits, n_local, half), f32),
                       pltpu.VMEM((row_size, 2, kd // LANES, LANES), f32)),
            in_specs=[hbm] * 4,
            out_specs=(vmem, vmem),
            scratch_shapes=[
                pltpu.SMEM((sweeps,), f32),
                pltpu.VMEM((n_rows, full_dim), bf16),
                pltpu.VMEM((fits, n_local), f32),
                pltpu.VMEM((nx, cp, half), bf16),
                pltpu.VMEM((kd, half), f32),
                pltpu.VMEM((kd, half), bf16),
                pltpu.VMEM((kd, LANES), f32),
                pltpu.VMEM((nx, kd, cp), f32),
                pltpu.VMEM((kd, cp), bf16),
                pltpu.VMEM((kd, half), f32),
                pltpu.VMEM((kd, LANES), f32),
                pltpu.VMEM((sweeps, nx, 2, srows, LANES), f32),
                pltpu.VMEM((sweeps, nx, n_peer, 2, srows, LANES), f32),
                pltpu.VMEM((2, kd // LANES, LANES), f32),
                pltpu.VMEM((kd // LANES, LANES), f32),
                pltpu.VMEM((2, kd, half), bf16),
                pltpu.VMEM((2, kd // LANES, LANES), f32),
                pltpu.VMEM((2, kd, LANES), f32),
                pltpu.VMEM((nx, 2, kd // 2, cp), f32),
                pltpu.VMEM((nx, 2, kd // 2, cp), f32),
                pltpu.VMEM((nx, 2, kd // 2, cp), bf16),
                pltpu.VMEM((2, kd // 2, half), f32),
                pltpu.VMEM((2, kd // 2, LANES), f32),
                dma((4,)), dma, dma((nx,)),
                dma((sweeps, nx)), dma((sweeps, nx)),
                dma, dma,
                dma((2, 2)), dma((2, 2)), dma((2,)), dma((2,)),
                dma((2, nh)), dma((2, nh)), dma((7 + 2 * nh,)), dma((7 + 2 * nh,)),
            ],
            compiler_params=pltpu.CompilerParams(collective_id=0, has_side_effects=True,
                                                 vmem_limit_bytes=48 * 1024 * 1024),
        )(*[pltpu.with_memory_space_constraint(v, pltpu.HBM) for v in (inv_temp, x_local, mu_init, logpi_init)])
        return pl.pallas_call(
            functools.partial(finish_kernel, fits),
            out_shape=(jax.ShapeDtypeStruct((fits, n_local, half), f32),
                       jax.ShapeDtypeStruct((fits, n_local), f32),
                       jax.ShapeDtypeStruct((fits, n_rows), f32)),
            in_specs=[pl.BlockSpec(memory_space=pl.ANY), vmem],
            out_specs=(hbm, vmem, vmem),
            scratch_shapes=[dma],
            compiler_params=pltpu.CompilerParams(vmem_limit_bytes=8 * 1024 * 1024),
        )(pltpu.with_memory_space_constraint(mu, pltpu.VMEM), pltpu.with_memory_space_constraint(small, pltpu.VMEM))

    return jax.shard_map(
        local_fit,
        mesh=mesh,
        in_specs=(P(("grp", "row"), None), P(None, ("grp", "comp"), None), P(None, ("grp", "comp")), P()),
        out_specs=(P(None, ("grp", "comp"), None), P(None, ("grp", "comp")), P(None, ("grp", "row"))),
        check_vma=False,
    )
```

```python
import functools
import math

import jax
import jax.numpy as jnp
from jax import lax
from jax.experimental import pallas as pl
from jax.experimental.pallas import tpu as pltpu
from jax.sharding import PartitionSpec as P

EPS_COUNT = 1e-6
PRIOR_ALPHA = 1e-3
LOG2E = math.log2(math.e)
LN2 = math.log(2.0)
LANES = 128
MESH = pl.DeviceIdType.MESH
NT = (((1,), (1,)), ((), ()))


def em_kernel(dims, beta_hbm, x_hbm, mu_hbm, logpi_hbm, mu_all, small_buf,
              beta_ref, x_ref, logpi_ref, xg, mu_f, mu_b, a_bc, lbuf, rb, s_acc, n_acc,
              stat_src, stat_buf, mx, small_src, a_row, xm_b, xa_row, xa_bc, xbuf_a, xbuf_b, xrb, xs_acc, xn_acc,
              loc_sem, x_send, x_recv, st_send, st_recv, sm_send, sm_recv,
              bk_send, bk_recv, ar_send, ar_recv, far_send, far_recv, sib_send, sib_recv):
    fits, n_comp, n_row, sweeps = dims["fits"], dims["comp"], dims["row"], dims["sweeps"]
    n_rows, half = x_ref.shape[0], mu_f.shape[1]
    nx = n_row // fits
    kd = mu_f.shape[0]
    cp = n_rows * fits
    lb = cp // LANES
    n_peer = n_comp * nx
    total_pts = n_rows * n_row
    total_comp = kd * nx * n_comp

    grp = lax.axis_index("grp")
    comp = lax.axis_index("comp")
    row = lax.axis_index("row")
    fit = lax.rem(row, fits)
    xi = row // fits
    me = comp * nx + xi

    def dev(c, r):
        return (grp, c, r)

    def hops(k):
        d_c, d_x = k // nx, k % nx
        return min(d_c, n_comp - d_c) + min(d_x, nx - d_x)

    peer_order = sorted(range(1, n_peer), key=lambda k: -hops(k))
    comp_at = [lax.rem(comp + d, n_comp) for d in range(n_comp)]
    row_at = [lax.rem(xi + d, nx) * fits + fit for d in range(nx)]

    def stat_peer(k):
        return dev(comp_at[k // nx], row_at[k % nx])

    barrier = pltpu.get_barrier_semaphore()
    n_sig = 0
    for k in peer_order:
        pl.semaphore_signal(barrier, inc=1, device_id=stat_peer(k), device_id_type=MESH)
        n_sig += 1
    for k in range(nx):
        for f in range(1, fits):
            x = lax.rem(xi + k, nx)
            pl.semaphore_signal(barrier, inc=1, device_id=dev(comp, x * fits + lax.rem(fit + f, fits)), device_id_type=MESH)
            n_sig += 1

    loads = [pltpu.make_async_copy(x_hbm, x_ref, loc_sem.at[0]),
             pltpu.make_async_copy(mu_hbm.at[fit, pl.ds(pl.multiple_of(xi * kd, kd), kd), :], mu_f, loc_sem.at[1]),
             pltpu.make_async_copy(logpi_hbm, logpi_ref, loc_sem.at[2]),
             pltpu.make_async_copy(beta_hbm, beta_ref, loc_sem.at[3])]
    for cpy in loads:
        cpy.start()

    def comp_terms(t, rows, mu, logw):
        beta = beta_ref[t]
        sq = jnp.sum(mu * mu, axis=1, keepdims=True)
        a = (logw - beta * sq) * LOG2E
        a_bc[rows, :] = jnp.broadcast_to(a, (a.shape[0], LANES))
        mu_b[rows, :] = mu.astype(jnp.bfloat16)

    loads[0].wait()
    with jax.named_scope("bar"):
        pl.semaphore_wait(barrier, n_sig)

    def x_cols(f):
        return pl.ds(pl.multiple_of(f * half, half), half)

    my_rows = pl.ds(pl.multiple_of(fit * n_rows, n_rows), n_rows)
    x_copies = []
    for k in (0, 1, 3, 2) if nx == 4 else range(nx):
        for f in range(fits):
            if k == 0 and f == 0:
                continue
            x = lax.rem(xi + k, nx)
            ft = lax.rem(fit + f, fits)
            cpy = pltpu.make_async_remote_copy(
                src_ref=x_ref.at[:, x_cols(ft)],
                dst_ref=xg.at[xi, my_rows],
                send_sem=x_send, recv_sem=x_recv.at[xi],
                device_id=dev(comp, x * fits + ft), device_id_type=MESH)
            cpy.start()
            x_copies.append(cpy)
    xg[xi, my_rows, :] = x_ref[:, x_cols(fit)]

    for cpy in loads[1:]:
        cpy.wait()
    for b in range(kd // LANES):
        rows = pl.ds(b * LANES, LANES)
        lw = logpi_ref[:, pl.ds(pl.multiple_of(xi * kd + b * LANES, LANES), LANES)]
        pick = lax.broadcasted_iota(jnp.int32, (fits, LANES), 0) == fit
        lw = jnp.sum(jnp.where(pick, lw, 0.0), axis=0, keepdims=True)
        lw = jnp.transpose(jnp.broadcast_to(lw, (LANES, LANES)))
        comp_terms(0, rows, mu_f[rows, :], lw[:, 0:1])
    for ref in (n_acc, s_acc, xn_acc, xs_acc):
        ref[...] = jnp.zeros(ref.shape, jnp.float32)

    def lanes_tile(v):
        return jnp.concatenate([v] * lb, axis=1)

    KB = 128
    nkb = kd // KB

    def e_dot(t, q):
        c2 = beta_ref[t] * (2.0 * LOG2E)
        with jax.named_scope("edot"):
            a = lax.dot_general(mu_b[...], xg[q], NT, preferred_element_type=jnp.float32)
            m8 = None
            for b in range(nkb):
                rows = slice(b * KB, (b + 1) * KB)
                l = a[rows, :] * c2 + lanes_tile(a_bc[rows, :])
                lbuf[q, rows, :] = l
                mb = jnp.max(l.reshape(KB // 8, 8, cp), axis=0)
                m8 = mb if m8 is None else jnp.maximum(m8, mb)
            mx[q] = m8

    def e_soft(t, q):
        m = jnp.max(mx[q], axis=0, keepdims=True)
        r8 = jnp.zeros((8, cp), jnp.float32)
        for b in range(nkb):
            rows = slice(b * KB, (b + 1) * KB)
            p = jnp.exp2(lbuf[q, rows, :] - m)
            lbuf[q, rows, :] = p
            r8 = r8 + jnp.sum(p.reshape(KB // 8, 8, cp), axis=0)
        r = jnp.sum(r8, axis=0, keepdims=True)
        for j in range(lb):
            cols = slice(j * LANES, (j + 1) * LANES)
            for ref in (stat_src.at[t, q], stat_buf.at[t, q, me]):
                ref[0, j:j + 1, :] = m[:, cols]
                ref[1, j:j + 1, :] = r[:, cols]

    def stat_copy(t, q, k):
        return pltpu.make_async_remote_copy(
            src_ref=stat_src.at[t, q], dst_ref=stat_buf.at[t, q, me],
            send_sem=st_send.at[t, q], recv_sem=st_recv.at[t, q],
            device_id=stat_peer(k), device_id_type=MESH)

    def stat_start(t, q):
        for k in peer_order:
            stat_copy(t, q, k).start()

    def stat_wait(t, q, send):
        part = stat_buf.at[t, q, pl.ds(0, n_peer - 1)]
        d = pltpu.make_async_copy(part, part, st_send.at[t, q] if send else st_recv.at[t, q])
        with jax.named_scope("stwait"):
            d.wait()

    def totals_of(t, q):
        m_all = stat_buf[t, q, :, 0]
        r_all = stat_buf[t, q, :, 1]
        m = jnp.max(m_all, axis=0)
        r = jnp.sum(r_all * jnp.exp2(m_all - m), axis=0)
        return m, r

    def scale_of(t, q):
        m, r = totals_of(t, q)
        return m, r, jnp.exp2(stat_src[t, q, 0] - m) / r

    def lane_rows(v, nrow):
        return jnp.concatenate([jnp.broadcast_to(v[j:j + 1, :], (nrow, LANES)) for j in range(lb)], axis=1)

    def m_rows(q, rows, nrow, sc):
        sc_row = jnp.concatenate([jnp.broadcast_to(sc[j:j + 1, :], (nrow, LANES)) for j in range(lb)], axis=1)
        res = lbuf[q, rows, :] * sc_row
        cnt = res[:, 0:LANES]
        for j in range(1, lb):
            cnt = cnt + res[:, j * LANES:(j + 1) * LANES]
        rb[rows, :] = res.astype(jnp.bfloat16)
        return cnt

    def m_chunk(t, q):
        m, r, sc = scale_of(t, q)
        with jax.named_scope("mchunk"):
            for b in range(nkb):
                rows = slice(b * KB, (b + 1) * KB)
                cnt = m_rows(q, rows, KB, sc)
                n_acc[rows, :] += cnt
            s_acc[...] += jnp.dot(rb[...], xg[q], preferred_element_type=jnp.float32)
        return m, r

    order = (0, 1, 3, 2) if nx == 4 else tuple(range(nx))
    for off in order:
        q = lax.rem(xi + off, nx)
        n_in = (fits - 1) if off == 0 else fits
        part = xg.at[q, pl.ds(0, n_in * n_rows)]
        with jax.named_scope("xwait"):
            pltpu.make_async_copy(part, part, x_recv.at[q]).wait()
        e_dot(0, q)
        with jax.named_scope("esoft"):
            e_soft(0, q)
        stat_start(0, q)

    right = lax.rem(xi + 1, nx)
    left = lax.rem(xi + nx - 1, nx)
    far = lax.rem(xi + 2, nx)
    sides = ((0, right), (1, left))

    kh = kd // 2
    nh = kh // KB

    def bulk_copy(d, x, h):
        rows = slice(h * kh, (h + 1) * kh)
        return pltpu.make_async_remote_copy(
            src_ref=mu_b.at[rows], dst_ref=xm_b.at[d, rows],
            send_sem=bk_send.at[d, h], recv_sem=bk_recv.at[d, h],
            device_id=dev(comp, x * fits + fit), device_id_type=MESH)

    def a_copy(d, x):
        return pltpu.make_async_remote_copy(
            src_ref=a_row, dst_ref=xa_row.at[d], send_sem=ar_send.at[d], recv_sem=ar_recv.at[d],
            device_id=dev(comp, x * fits + fit), device_id_type=MESH)

    def sweep(t, last):
        def m_body(q, c):
            stat_wait(t, q, False)
            m_chunk(t, q)
            return c

        lax.fori_loop(0, nx, m_body, 0)
        with jax.named_scope("terms"):
            for b in range(nkb):
                rows = slice(b * KB, (b + 1) * KB)
                cnt = jnp.sum(n_acc[rows, :], axis=1, keepdims=True)
                mu = s_acc[rows, :] / (cnt + EPS_COUNT)
                logw = jnp.log((cnt + PRIOR_ALPHA) / (total_pts + total_comp * PRIOR_ALPHA))
                comp_terms(t + 1, rows, mu, logw)
                n_acc[rows, :] = jnp.zeros((KB, LANES), jnp.float32)
                s_acc[rows, :] = jnp.zeros((KB, half), jnp.float32)
        if last:
            for d, x in sides:
                bulk_copy(d, x, d).start()
        e_dot(t + 1, 0)
        if last:
            for b in range(nkb):
                a_row[b:b + 1, :] = jnp.transpose(a_bc[b * KB:(b + 1) * KB, :])[0:1, :]
            for d, x in sides:
                a_copy(d, x).start()

        def e_body(q, c):
            e_dot(t + 1, q + 1)
            with jax.named_scope("esoft"):
                e_soft(t + 1, q)
            with jax.named_scope("stsend"):
                stat_start(t + 1, q)
            return c

        lax.fori_loop(0, nx - 1, e_body, 0)
        with jax.named_scope("esoft"):
            e_soft(t + 1, nx - 1)
        with jax.named_scope("stsend"):
            stat_start(t + 1, nx - 1)

    def sweep_body(t, c):
        sweep(t, False)
        return c

    lax.fori_loop(0, sweeps - 2, sweep_body, 0)
    sweep(sweeps - 2, True)

    tl = sweeps - 1

    sq_rows = []
    for j in range(lb):
        xb = xg[xi, j * LANES:(j + 1) * LANES, :].astype(jnp.float32)
        sq_rows.append(jnp.sum(jnp.transpose(xb * xb), axis=0, keepdims=True))
    sq = jnp.concatenate(sq_rows, axis=0)

    c2_last = beta_ref[tl] * (2.0 * LOG2E)
    sib = xi * fits + lax.rem(fit + 1, fits)

    for d, x in sides:
        bulk_copy(d, x, 1 - d).start()

    def x_ready(halves):
        with jax.named_scope("bulkwait"):
            for d, h in enumerate(halves):
                bulk_copy(d, left, h).wait_recv()

    def x_terms(halves):
        with jax.named_scope("xterms"):
            for d, h in enumerate(halves):
                for b in range(h * nh, (h + 1) * nh):
                    xa_bc[d, b * KB:(b + 1) * KB, :] = jnp.transpose(jnp.broadcast_to(xa_row[d, b:b + 1, :], (KB, LANES)))

    x_ready((0, 1))
    owner = (comp * nx + left, comp * nx + right)

    def x_dot(buf, q, halves):
        for d, h in enumerate(halves):
            a = lax.dot_general(xm_b[d, h * kh:(h + 1) * kh, :], xg[q], NT, preferred_element_type=jnp.float32)
            for b in range(nh):
                rows = slice(b * KB, (b + 1) * KB)
                buf[d, rows, :] = a[rows, :] * c2_last + lanes_tile(xa_bc[d, h * kh + b * KB:h * kh + (b + 1) * KB, :])

    def x_scales(q):
        m, r = totals_of(tl, q)
        res = []
        for d in range(2):
            m_j = stat_buf[tl, q, owner[d], 0]
            res.append((lane_rows(m_j, KB), lane_rows(jnp.exp2(m_j - m) / r, KB)))
        return res

    def x_resp(buf, q, s_at, d, h, scales):
        m_row, sc_row = scales[d]
        for b in range(nh):
            rows = slice(b * KB, (b + 1) * KB)
            res = jnp.exp2(buf[d, rows, :] - m_row) * sc_row
            cnt = res[:, 0:LANES]
            for j in range(1, lb):
                cnt = cnt + res[:, j * LANES:(j + 1) * LANES]
            xrb[q, d, rows, :] = res.astype(jnp.bfloat16)
            xn_acc[s_at, d, rows, :] += cnt

    def x_sum(q, s_at, d):
        xs_acc[s_at, d] += jnp.dot(xrb[q, d], xg[q], preferred_element_type=jnp.float32)

    def x_units(buf, q, s_at, halves):
        scales = x_scales(q)
        for d, h in enumerate(halves):
            x_resp(buf, q, s_at, d, h, scales)
            x_sum(q, s_at, d)

    def mean_rows(na, sa):
        return sa / (jnp.sum(na, axis=1, keepdims=True) + EPS_COUNT)

    def span(x, start, size):
        return pl.ds(pl.multiple_of(x * kd + start, KB), size)

    waits = []

    def push(x, start, size, send_sem, recv_sem, r):
        part = mu_all.at[fit, span(x, start, size)]
        cpy = pltpu.make_async_remote_copy(src_ref=part, dst_ref=part, send_sem=send_sem, recv_sem=recv_sem,
                                           device_id=dev(comp, r), device_id_type=MESH)
        cpy.start()
        waits.append(cpy.wait_send)

    def x_finish(s_at, d, h, b):
        x = (left, right)[d]
        rows = slice(b * KB, (b + 1) * KB)
        mu_all[fit, span(x, h * kh + b * KB, KB), :] = mean_rows(xn_acc[s_at, d, rows, :], xs_acc[s_at, d, rows, :])

    with jax.named_scope("arwait"):
        for d in range(2):
            a_copy(d, left).wait_recv()
    x_terms((0, 1))
    x_terms((1, 0))
    with jax.named_scope("xdotA"):
        for q in range(nx):
            x_dot(xbuf_a.at[q], q, (0, 1))

    def x_last(buf, q, s_at, halves, done):
        scales = x_scales(q)
        for d, h in enumerate(halves):
            x_resp(buf, q, s_at, d, h, scales)
            x_sum(q, s_at, d)
            for b in range(nh):
                x_finish(s_at, d, h, b)
            for b in range(nh):
                done(d, h, b)

    def xa_body(q, c):
        stat_wait(tl, q, False)
        with jax.named_scope("xunitA"):
            x_units(xbuf_a.at[q], q, 0, (0, 1))
        m_chunk(tl, q)
        return c

    lax.fori_loop(0, nx - 2, xa_body, 0)
    stat_wait(tl, nx - 2, False)
    with jax.named_scope("xunitA"):
        x_units(xbuf_a.at[nx - 2], nx - 2, 0, (0, 1))
    ql = nx - 1
    stat_wait(tl, ql, False)

    def a_done(d, h, b):
        x = (left, right)[d]
        push(x, h * kh + b * KB, KB, far_send.at[d, b], far_recv.at[d, b], sides[d][1] * fits + fit)
        if b == nh - 1:
            push(x, h * kh, kh, sib_send.at[d], sib_recv.at[d], sib)

    with jax.named_scope("xfinA"):
        x_last(xbuf_a.at[ql], ql, 0, (0, 1), a_done)
    m_chunk(tl, nx - 2)
    m_chunk(tl, ql)
    with jax.named_scope("ownfin"):
        m, r, _ = scale_of(tl, xi)
        small_src[1, 0:lb, :] = m * LN2 + jnp.log(r) - beta_ref[tl] * sq
        for b in range(nkb):
            rows = slice(b * KB, (b + 1) * KB)
            na = n_acc[rows, :]
            mu_all[fit, span(xi, b * KB, KB), :] = mean_rows(na, s_acc[rows, :])
            n_row_v = jnp.sum(jnp.transpose(na), axis=0, keepdims=True)
            small_src[0, b:b + 1, :] = jnp.log((n_row_v + PRIOR_ALPHA) / (total_pts + total_comp * PRIOR_ALPHA))
        push(xi, 0, kd, sib_send.at[2], sib_recv.at[2], sib)
        for k in range(1, n_row):
            r = lax.rem(row + k, n_row)
            cpy = pltpu.make_async_remote_copy(src_ref=small_src, dst_ref=small_buf.at[row], send_sem=sm_send, recv_sem=sm_recv,
                                               device_id=dev(comp, r), device_id_type=MESH)
            cpy.start()
        small_buf[row] = small_src[...]

    x_ready((1, 0))
    with jax.named_scope("xunitB"):
        x_dot(xbuf_b.at[0], 0, (1, 0))
        for q in range(nx - 1):
            x_dot(xbuf_b.at[q + 1], q + 1, (1, 0))
            scales = x_scales(q)
            for d, h in enumerate((1, 0)):
                x_resp(xbuf_b.at[q], q, 1, d, h, scales)
            if q > 0:
                for d in range(2):
                    x_sum(q - 1, 1, d)
        for d in range(2):
            x_sum(nx - 2, 1, d)

    def b_done(d, h, b):
        if b % 2:
            k = 3 + 2 * d + b // 2
            push((left, right)[d], h * kh + (b - 1) * KB, 2 * KB, sib_send.at[k], sib_recv.at[k], sib)

    with jax.named_scope("xfinB"):
        x_last(xbuf_b.at[ql], ql, 1, (1, 0), b_done)

    with jax.named_scope("farwait"):
        for b in range(nh):
            for d in range(2):
                part = mu_all.at[fit, span(far, d * kh + b * KB, KB)]
                pltpu.make_async_copy(part, part, far_recv.at[d, b]).wait()
                k = 7 + d * nh + b
                push(far, d * kh + b * KB, KB, sib_send.at[k], sib_recv.at[k], sib)
    ofit = lax.rem(fit + 1, fits)

    def sib_wait(x, start, size, k):
        part = mu_all.at[ofit, span(x, start, size)]
        pltpu.make_async_copy(part, part, sib_recv.at[k]).wait()

    with jax.named_scope("sibwait"):
        sib_wait(xi, 0, kd, 2)
        for d, x in ((0, left), (1, right)):
            sib_wait(x, d * kh, kh, d)
            sib_wait(x, (1 - d) * kh, kh // 2, 3 + 2 * d)
            sib_wait(x, (1 - d) * kh + kh // 2, kh // 2, 4 + 2 * d)
            for b in range(nh):
                sib_wait(far, d * kh + b * KB, KB, 7 + d * nh + b)

    part = small_buf.at[pl.ds(0, n_row - 1)]
    pltpu.make_async_copy(part, part, sm_recv).wait()
    pltpu.make_async_copy(part, part, sm_send).wait()
    for w in waits:
        w()
    def drain(t, c):
        for q in range(nx):
            stat_wait(t, q, True)
        return c
    lax.fori_loop(0, sweeps, drain, 0)
    for cpy in x_copies:
        cpy.wait_send()
    for d in range(2):
        bulk_copy(d, left, 0).wait_send()
        bulk_copy(d, left, 1).wait_send()
        a_copy(d, left).wait_send()


def finish_kernel(fits, mu_all, small, o_mu, o_logpi, o_lse, logpi_buf, lse_buf, sems):
    row = lax.axis_index("row")
    fit = lax.rem(row, fits)
    first = row - fit
    n_row = small.shape[0]
    nx = n_row // fits
    kd = o_logpi.shape[1] // nx
    per = o_lse.shape[1] // LANES
    parts = 4
    step = mu_all.shape[1] // parts
    copies = []
    for f in range(fits):
        for p in range(parts):
            part = pl.ds(p * step, step)
            copies.append(pltpu.make_async_copy(mu_all.at[f, part], o_mu.at[f, part], sems.at[f * parts + p]))
            copies[-1].start()
    for f in range(fits):
        for j in range(per):
            v = small[first + f, 1, j:j + 1, :]
            for g in range(1, fits):
                v = jnp.where(fit == g, small[first + f, 1, g * per + j:g * per + j + 1, :], v)
            lse_buf[f:f + 1, j * LANES:(j + 1) * LANES] = v
        for x in range(nx):
            for j in range(kd // LANES):
                logpi_buf[f:f + 1, x * kd + j * LANES:x * kd + (j + 1) * LANES] = small[x * fits + f, 0, j:j + 1, :]
    n = fits * parts
    for k, (src, dst) in enumerate(((logpi_buf, o_logpi), (lse_buf, o_lse))):
        copies.append(pltpu.make_async_copy(src, dst, sems.at[n + k]))
        copies[-1].start()
    for c in copies:
        c.wait()


def solution(mesh):
    comp_size = mesh.shape["comp"]
    row_size = mesh.shape["row"]

    def local_fit(x_local, mu_init, logpi_init, inv_temp):
        n_rows, full_dim = x_local.shape
        fits, n_local, half = mu_init.shape
        sweeps = inv_temp.shape[0]
        nx = row_size // fits
        kd = n_local // nx
        cp = n_rows * fits
        n_peer = comp_size * nx
        kb = LANES
        nh = kd // 2 // kb
        dims = {"fits": fits, "comp": comp_size, "row": row_size, "sweeps": sweeps}
        f32, bf16 = jnp.float32, jnp.bfloat16
        dma = pltpu.SemaphoreType.DMA
        srows = cp // LANES
        hbm = pl.BlockSpec(memory_space=pltpu.HBM)
        vmem = pl.BlockSpec(memory_space=pltpu.VMEM)
        mu, small = pl.pallas_call(
            functools.partial(em_kernel, dims),
            out_shape=(pltpu.VMEM((fits, n_local, half), f32),
                       pltpu.VMEM((row_size, 2, kd // LANES, LANES), f32)),
            in_specs=[hbm] * 4,
            out_specs=(vmem, vmem),
            scratch_shapes=[
                pltpu.SMEM((sweeps,), f32),
                pltpu.VMEM((n_rows, full_dim), bf16),
                pltpu.VMEM((fits, n_local), f32),
                pltpu.VMEM((nx, cp, half), bf16),
                pltpu.VMEM((kd, half), f32),
                pltpu.VMEM((kd, half), bf16),
                pltpu.VMEM((kd, LANES), f32),
                pltpu.VMEM((nx, kd, cp), f32),
                pltpu.VMEM((kd, cp), bf16),
                pltpu.VMEM((kd, half), f32),
                pltpu.VMEM((kd, LANES), f32),
                pltpu.VMEM((sweeps, nx, 2, srows, LANES), f32),
                pltpu.VMEM((sweeps, nx, n_peer, 2, srows, LANES), f32),
                pltpu.VMEM((nx, 8, cp), f32),
                pltpu.VMEM((2, kd // LANES, LANES), f32),
                pltpu.VMEM((kd // LANES, LANES), f32),
                pltpu.VMEM((2, kd, half), bf16),
                pltpu.VMEM((2, kd // LANES, LANES), f32),
                pltpu.VMEM((2, kd, LANES), f32),
                pltpu.VMEM((nx, 2, kd // 2, cp), f32),
                pltpu.VMEM((nx, 2, kd // 2, cp), f32),
                pltpu.VMEM((nx, 2, kd // 2, cp), bf16),
                pltpu.VMEM((2, 2, kd // 2, half), f32),
                pltpu.VMEM((2, 2, kd // 2, LANES), f32),
                dma((4,)), dma, dma((nx,)),
                dma((sweeps, nx)), dma((sweeps, nx)),
                dma, dma,
                dma((2, 2)), dma((2, 2)), dma((2,)), dma((2,)),
                dma((2, nh)), dma((2, nh)), dma((7 + 2 * nh,)), dma((7 + 2 * nh,)),
            ],
            compiler_params=pltpu.CompilerParams(collective_id=0, has_side_effects=True,
                                                 vmem_limit_bytes=48 * 1024 * 1024),
        )(*[pltpu.with_memory_space_constraint(v, pltpu.HBM) for v in (inv_temp, x_local, mu_init, logpi_init)])
        return pl.pallas_call(
            functools.partial(finish_kernel, fits),
            out_shape=(jax.ShapeDtypeStruct((fits, n_local, half), f32),
                       jax.ShapeDtypeStruct((fits, n_local), f32),
                       jax.ShapeDtypeStruct((fits, n_rows), f32)),
            in_specs=[pl.BlockSpec(memory_space=pl.ANY), vmem],
            out_specs=(hbm, hbm, hbm),
            scratch_shapes=[pltpu.VMEM((fits, n_local), f32), pltpu.VMEM((fits, n_rows), f32), dma((4 * fits + 2,))],
            compiler_params=pltpu.CompilerParams(vmem_limit_bytes=8 * 1024 * 1024),
        )(pltpu.with_memory_space_constraint(mu, pltpu.VMEM), pltpu.with_memory_space_constraint(small, pltpu.VMEM))

    return jax.shard_map(
        local_fit,
        mesh=mesh,
        in_specs=(P(("grp", "row"), None), P(None, ("grp", "comp"), None), P(None, ("grp", "comp")), P()),
        out_specs=(P(None, ("grp", "comp"), None), P(None, ("grp", "comp")), P(None, ("grp", "row"))),
        check_vma=False,
    )
```

```python
import functools
import math

import jax
import jax.numpy as jnp
from jax import lax
from jax.experimental import pallas as pl
from jax.experimental.pallas import tpu as pltpu
from jax.sharding import PartitionSpec as P

EPS_COUNT = 1e-6
PRIOR_ALPHA = 1e-3
LOG2E = math.log2(math.e)
LN2 = math.log(2.0)
LANES = 128
MESH = pl.DeviceIdType.MESH
NT = (((1,), (1,)), ((), ()))


def em_kernel(dims, beta_hbm, x_hbm, mu_hbm, logpi_hbm, mu_all, small_buf,
              beta_ref, x_ref, logpi_ref, xg, mu_f, mu_b, a_bc, lbuf, rb, s_acc, n_acc,
              stat_src, stat_buf, mx, small_src, a_row, xm_b, xa_row, xa_bc, xbuf_a, xbuf_b, xrb, xs_acc, xn_acc,
              loc_sem, x_send, x_recv, st_send, st_recv, sm_send, sm_recv,
              bk_send, bk_recv, ar_send, ar_recv, far_send, far_recv, sib_send, sib_recv):
    fits, n_comp, n_row, sweeps = dims["fits"], dims["comp"], dims["row"], dims["sweeps"]
    n_rows, half = x_ref.shape[0], mu_f.shape[1]
    nx = n_row // fits
    kd = mu_f.shape[0]
    cp = n_rows * fits
    lb = cp // LANES
    n_peer = n_comp * nx
    total_pts = n_rows * n_row
    total_comp = kd * nx * n_comp

    grp = lax.axis_index("grp")
    comp = lax.axis_index("comp")
    row = lax.axis_index("row")
    fit = lax.rem(row, fits)
    xi = row // fits
    me = comp * nx + xi

    def dev(c, r):
        return (grp, c, r)

    def hops(k):
        d_c, d_x = k // nx, k % nx
        return min(d_c, n_comp - d_c) + min(d_x, nx - d_x)

    peer_order = sorted(range(1, n_peer), key=lambda k: -hops(k))
    comp_at = [lax.rem(comp + d, n_comp) for d in range(n_comp)]
    row_at = [lax.rem(xi + d, nx) * fits + fit for d in range(nx)]

    def stat_peer(k):
        return dev(comp_at[k // nx], row_at[k % nx])

    barrier = pltpu.get_barrier_semaphore()
    n_sig = 0
    for k in peer_order:
        pl.semaphore_signal(barrier, inc=1, device_id=stat_peer(k), device_id_type=MESH)
        n_sig += 1
    for k in range(nx):
        for f in range(1, fits):
            x = lax.rem(xi + k, nx)
            pl.semaphore_signal(barrier, inc=1, device_id=dev(comp, x * fits + lax.rem(fit + f, fits)), device_id_type=MESH)
            n_sig += 1

    loads = [pltpu.make_async_copy(x_hbm, x_ref, loc_sem.at[0]),
             pltpu.make_async_copy(mu_hbm.at[fit, pl.ds(pl.multiple_of(xi * kd, kd), kd), :], mu_f, loc_sem.at[1]),
             pltpu.make_async_copy(logpi_hbm, logpi_ref, loc_sem.at[2]),
             pltpu.make_async_copy(beta_hbm, beta_ref, loc_sem.at[3])]
    for cpy in loads:
        cpy.start()

    def comp_terms(t, rows, mu, logw):
        beta = beta_ref[t]
        sq = jnp.sum(mu * mu, axis=1, keepdims=True)
        a = (logw - beta * sq) * LOG2E
        a_bc[rows, :] = jnp.broadcast_to(a, (a.shape[0], LANES))
        mu_b[rows, :] = mu.astype(jnp.bfloat16)

    loads[0].wait()
    with jax.named_scope("bar"):
        pl.semaphore_wait(barrier, n_sig)

    def x_cols(f):
        return pl.ds(pl.multiple_of(f * half, half), half)

    my_rows = pl.ds(pl.multiple_of(fit * n_rows, n_rows), n_rows)
    x_copies = []
    for k in (0, 1, 3, 2) if nx == 4 else range(nx):
        for f in range(fits):
            if k == 0 and f == 0:
                continue
            x = lax.rem(xi + k, nx)
            ft = lax.rem(fit + f, fits)
            cpy = pltpu.make_async_remote_copy(
                src_ref=x_ref.at[:, x_cols(ft)],
                dst_ref=xg.at[xi, my_rows],
                send_sem=x_send, recv_sem=x_recv.at[xi],
                device_id=dev(comp, x * fits + ft), device_id_type=MESH)
            cpy.start()
            x_copies.append(cpy)
    xg[xi, my_rows, :] = x_ref[:, x_cols(fit)]

    for cpy in loads[1:]:
        cpy.wait()
    for b in range(kd // LANES):
        rows = pl.ds(b * LANES, LANES)
        lw = logpi_ref[:, pl.ds(pl.multiple_of(xi * kd + b * LANES, LANES), LANES)]
        pick = lax.broadcasted_iota(jnp.int32, (fits, LANES), 0) == fit
        lw = jnp.sum(jnp.where(pick, lw, 0.0), axis=0, keepdims=True)
        lw = jnp.transpose(jnp.broadcast_to(lw, (LANES, LANES)))
        comp_terms(0, rows, mu_f[rows, :], lw[:, 0:1])
    for ref in (n_acc, s_acc, xn_acc, xs_acc):
        ref[...] = jnp.zeros(ref.shape, jnp.float32)

    def lanes_tile(v):
        return jnp.concatenate([v] * lb, axis=1)

    KB = 128
    nkb = kd // KB

    def e_dot(t, q):
        c2 = beta_ref[t] * (2.0 * LOG2E)
        with jax.named_scope("edot"):
            a = lax.dot_general(mu_b[...], xg[q], NT, preferred_element_type=jnp.float32)
            m8 = None
            for b in range(nkb):
                rows = slice(b * KB, (b + 1) * KB)
                l = a[rows, :] * c2 + lanes_tile(a_bc[rows, :])
                lbuf[q, rows, :] = l
                mb = jnp.max(l.reshape(KB // 8, 8, cp), axis=0)
                m8 = mb if m8 is None else jnp.maximum(m8, mb)
            mx[q] = m8

    def e_soft(t, q):
        m = jnp.max(mx[q], axis=0, keepdims=True)
        r8 = jnp.zeros((8, cp), jnp.float32)
        for b in range(nkb):
            rows = slice(b * KB, (b + 1) * KB)
            p = jnp.exp2(lbuf[q, rows, :] - m)
            lbuf[q, rows, :] = p
            r8 = r8 + jnp.sum(p.reshape(KB // 8, 8, cp), axis=0)
        r = jnp.sum(r8, axis=0, keepdims=True)
        for j in range(lb):
            cols = slice(j * LANES, (j + 1) * LANES)
            for ref in (stat_src.at[t, q], stat_buf.at[t, q, me]):
                ref[0, j:j + 1, :] = m[:, cols]
                ref[1, j:j + 1, :] = r[:, cols]

    def stat_copy(t, q, k):
        return pltpu.make_async_remote_copy(
            src_ref=stat_src.at[t, q], dst_ref=stat_buf.at[t, q, me],
            send_sem=st_send.at[t, q], recv_sem=st_recv.at[t, q],
            device_id=stat_peer(k), device_id_type=MESH)

    def stat_start(t, q):
        for k in peer_order:
            stat_copy(t, q, k).start()

    def stat_wait(t, q, send):
        part = stat_buf.at[t, q, pl.ds(0, n_peer - 1)]
        d = pltpu.make_async_copy(part, part, st_send.at[t, q] if send else st_recv.at[t, q])
        with jax.named_scope("stwait"):
            d.wait()

    def totals_of(t, q):
        m_all = stat_buf[t, q, :, 0]
        r_all = stat_buf[t, q, :, 1]
        m = jnp.max(m_all, axis=0)
        r = jnp.sum(r_all * jnp.exp2(m_all - m), axis=0)
        return m, r

    def scale_of(t, q):
        m, r = totals_of(t, q)
        return m, r, jnp.exp2(stat_src[t, q, 0] - m) / r

    def lane_rows(v, nrow):
        return jnp.concatenate([jnp.broadcast_to(v[j:j + 1, :], (nrow, LANES)) for j in range(lb)], axis=1)

    def m_rows(q, rows, nrow, sc):
        sc_row = jnp.concatenate([jnp.broadcast_to(sc[j:j + 1, :], (nrow, LANES)) for j in range(lb)], axis=1)
        res = lbuf[q, rows, :] * sc_row
        cnt = res[:, 0:LANES]
        for j in range(1, lb):
            cnt = cnt + res[:, j * LANES:(j + 1) * LANES]
        rb[rows, :] = res.astype(jnp.bfloat16)
        return cnt

    def m_chunk(t, q):
        m, r, sc = scale_of(t, q)
        with jax.named_scope("mchunk"):
            for b in range(nkb):
                rows = slice(b * KB, (b + 1) * KB)
                cnt = m_rows(q, rows, KB, sc)
                n_acc[rows, :] += cnt
            s_acc[...] += jnp.dot(rb[...], xg[q], preferred_element_type=jnp.float32)
        return m, r

    order = (0, 1, 3, 2) if nx == 4 else tuple(range(nx))
    for off in order:
        q = lax.rem(xi + off, nx)
        n_in = (fits - 1) if off == 0 else fits
        part = xg.at[q, pl.ds(0, n_in * n_rows)]
        with jax.named_scope("xwait"):
            pltpu.make_async_copy(part, part, x_recv.at[q]).wait()
        e_dot(0, q)
        with jax.named_scope("esoft"):
            e_soft(0, q)
        stat_start(0, q)

    right = lax.rem(xi + 1, nx)
    left = lax.rem(xi + nx - 1, nx)
    far = lax.rem(xi + 2, nx)
    sides = ((0, right), (1, left))

    kh = kd // 2
    nh = kh // KB

    def bulk_copy(d, x, h):
        rows = slice(h * kh, (h + 1) * kh)
        return pltpu.make_async_remote_copy(
            src_ref=mu_b.at[rows], dst_ref=xm_b.at[d, rows],
            send_sem=bk_send.at[d, h], recv_sem=bk_recv.at[d, h],
            device_id=dev(comp, x * fits + fit), device_id_type=MESH)

    def a_copy(d, x):
        return pltpu.make_async_remote_copy(
            src_ref=a_row, dst_ref=xa_row.at[d], send_sem=ar_send.at[d], recv_sem=ar_recv.at[d],
            device_id=dev(comp, x * fits + fit), device_id_type=MESH)

    def sweep(t, last):
        def m_body(q, c):
            stat_wait(t, q, False)
            m_chunk(t, q)
            return c

        lax.fori_loop(0, nx, m_body, 0)
        with jax.named_scope("terms"):
            for b in range(nkb):
                rows = slice(b * KB, (b + 1) * KB)
                cnt = jnp.sum(n_acc[rows, :], axis=1, keepdims=True)
                mu = s_acc[rows, :] / (cnt + EPS_COUNT)
                logw = jnp.log((cnt + PRIOR_ALPHA) / (total_pts + total_comp * PRIOR_ALPHA))
                comp_terms(t + 1, rows, mu, logw)
                n_acc[rows, :] = jnp.zeros((KB, LANES), jnp.float32)
                s_acc[rows, :] = jnp.zeros((KB, half), jnp.float32)
        if last:
            for d, x in sides:
                bulk_copy(d, x, d).start()
        e_dot(t + 1, 0)
        if last:
            for b in range(nkb):
                a_row[b:b + 1, :] = jnp.transpose(a_bc[b * KB:(b + 1) * KB, :])[0:1, :]
            for d, x in sides:
                a_copy(d, x).start()

        def e_body(q, c):
            with jax.named_scope("esoft"):
                e_soft(t + 1, q)
            with jax.named_scope("stsend"):
                stat_start(t + 1, q)
            e_dot(t + 1, q + 1)
            return c

        lax.fori_loop(0, nx - 1, e_body, 0)
        with jax.named_scope("esoft"):
            e_soft(t + 1, nx - 1)
        with jax.named_scope("stsend"):
            stat_start(t + 1, nx - 1)

    def sweep_body(t, c):
        sweep(t, False)
        return c

    lax.fori_loop(0, sweeps - 2, sweep_body, 0)
    sweep(sweeps - 2, True)

    tl = sweeps - 1

    sq_rows = []
    for j in range(lb):
        xb = xg[xi, j * LANES:(j + 1) * LANES, :].astype(jnp.float32)
        sq_rows.append(jnp.sum(jnp.transpose(xb * xb), axis=0, keepdims=True))
    sq = jnp.concatenate(sq_rows, axis=0)

    c2_last = beta_ref[tl] * (2.0 * LOG2E)
    sib = xi * fits + lax.rem(fit + 1, fits)

    for d, x in sides:
        bulk_copy(d, x, 1 - d).start()

    def x_ready(halves):
        with jax.named_scope("bulkwait"):
            for d, h in enumerate(halves):
                bulk_copy(d, left, h).wait_recv()

    def x_terms(halves):
        with jax.named_scope("xterms"):
            for d, h in enumerate(halves):
                for b in range(h * nh, (h + 1) * nh):
                    xa_bc[d, b * KB:(b + 1) * KB, :] = jnp.transpose(jnp.broadcast_to(xa_row[d, b:b + 1, :], (KB, LANES)))

    x_ready((0, 1))
    owner = (comp * nx + left, comp * nx + right)

    def x_dot(buf, q, halves):
        for d, h in enumerate(halves):
            a = lax.dot_general(xm_b[d, h * kh:(h + 1) * kh, :], xg[q], NT, preferred_element_type=jnp.float32)
            for b in range(nh):
                rows = slice(b * KB, (b + 1) * KB)
                buf[d, rows, :] = a[rows, :] * c2_last + lanes_tile(xa_bc[d, h * kh + b * KB:h * kh + (b + 1) * KB, :])

    def x_scales(q):
        m, r = totals_of(tl, q)
        res = []
        for d in range(2):
            m_j = stat_buf[tl, q, owner[d], 0]
            res.append((lane_rows(m_j, KB), lane_rows(jnp.exp2(m_j - m) / r, KB)))
        return res

    def x_resp(buf, q, s_at, d, h, scales):
        m_row, sc_row = scales[d]
        for b in range(nh):
            rows = slice(b * KB, (b + 1) * KB)
            res = jnp.exp2(buf[d, rows, :] - m_row) * sc_row
            cnt = res[:, 0:LANES]
            for j in range(1, lb):
                cnt = cnt + res[:, j * LANES:(j + 1) * LANES]
            xrb[q, d, rows, :] = res.astype(jnp.bfloat16)
            xn_acc[s_at, d, rows, :] += cnt

    def x_sum(q, s_at, d):
        xs_acc[s_at, d] += jnp.dot(xrb[q, d], xg[q], preferred_element_type=jnp.float32)

    def x_units(buf, q, s_at, halves):
        scales = x_scales(q)
        for d, h in enumerate(halves):
            x_resp(buf, q, s_at, d, h, scales)
            x_sum(q, s_at, d)

    def mean_rows(na, sa):
        return sa / (jnp.sum(na, axis=1, keepdims=True) + EPS_COUNT)

    def span(x, start, size):
        return pl.ds(pl.multiple_of(x * kd + start, KB), size)

    waits = []

    def push(x, start, size, send_sem, recv_sem, r):
        part = mu_all.at[fit, span(x, start, size)]
        cpy = pltpu.make_async_remote_copy(src_ref=part, dst_ref=part, send_sem=send_sem, recv_sem=recv_sem,
                                           device_id=dev(comp, r), device_id_type=MESH)
        cpy.start()
        waits.append(cpy.wait_send)

    def x_finish(s_at, d, h, b):
        x = (left, right)[d]
        rows = slice(b * KB, (b + 1) * KB)
        mu_all[fit, span(x, h * kh + b * KB, KB), :] = mean_rows(xn_acc[s_at, d, rows, :], xs_acc[s_at, d, rows, :])

    with jax.named_scope("arwait"):
        for d in range(2):
            a_copy(d, left).wait_recv()
    x_terms((0, 1))
    x_terms((1, 0))
    with jax.named_scope("xdotA"):
        for q in range(nx):
            x_dot(xbuf_a.at[q], q, (0, 1))

    def x_last(buf, q, s_at, halves, done):
        scales = x_scales(q)
        for d, h in enumerate(halves):
            x_resp(buf, q, s_at, d, h, scales)
            x_sum(q, s_at, d)
            for b in range(nh):
                x_finish(s_at, d, h, b)
            for b in range(nh):
                done(d, h, b)

    def xa_body(q, c):
        stat_wait(tl, q, False)
        with jax.named_scope("xunitA"):
            x_units(xbuf_a.at[q], q, 0, (0, 1))
        return c

    lax.fori_loop(0, nx - 2, xa_body, 0)
    stat_wait(tl, nx - 2, False)
    with jax.named_scope("xunitA"):
        x_units(xbuf_a.at[nx - 2], nx - 2, 0, (0, 1))
    ql = nx - 1
    stat_wait(tl, ql, False)

    def a_done(d, h, b):
        x = (left, right)[d]
        push(x, h * kh + b * KB, KB, far_send.at[d, b], far_recv.at[d, b], sides[d][1] * fits + fit)
        if b == nh - 1:
            push(x, h * kh, kh, sib_send.at[d], sib_recv.at[d], sib)

    with jax.named_scope("xfinA"):
        x_last(xbuf_a.at[ql], ql, 0, (0, 1), a_done)

    def own_body(q, c):
        m_chunk(tl, q)
        return c

    lax.fori_loop(0, nx, own_body, 0)
    with jax.named_scope("ownfin"):
        m, r, _ = scale_of(tl, xi)
        small_src[1, 0:lb, :] = m * LN2 + jnp.log(r) - beta_ref[tl] * sq
        for b in range(nkb):
            rows = slice(b * KB, (b + 1) * KB)
            na = n_acc[rows, :]
            mu_all[fit, span(xi, b * KB, KB), :] = mean_rows(na, s_acc[rows, :])
            n_row_v = jnp.sum(jnp.transpose(na), axis=0, keepdims=True)
            small_src[0, b:b + 1, :] = jnp.log((n_row_v + PRIOR_ALPHA) / (total_pts + total_comp * PRIOR_ALPHA))
        push(xi, 0, kd, sib_send.at[2], sib_recv.at[2], sib)
        for k in range(1, n_row):
            r = lax.rem(row + k, n_row)
            cpy = pltpu.make_async_remote_copy(src_ref=small_src, dst_ref=small_buf.at[row], send_sem=sm_send, recv_sem=sm_recv,
                                               device_id=dev(comp, r), device_id_type=MESH)
            cpy.start()
        small_buf[row] = small_src[...]

    x_ready((1, 0))
    with jax.named_scope("xunitB"):
        x_dot(xbuf_b.at[0], 0, (1, 0))
        for q in range(nx - 1):
            x_dot(xbuf_b.at[q + 1], q + 1, (1, 0))
            scales = x_scales(q)
            for d, h in enumerate((1, 0)):
                x_resp(xbuf_b.at[q], q, 1, d, h, scales)
            if q > 0:
                for d in range(2):
                    x_sum(q - 1, 1, d)
        for d in range(2):
            x_sum(nx - 2, 1, d)

    def b_done(d, h, b):
        if b % 2:
            k = 3 + 2 * d + b // 2
            push((left, right)[d], h * kh + (b - 1) * KB, 2 * KB, sib_send.at[k], sib_recv.at[k], sib)

    with jax.named_scope("xfinB"):
        x_last(xbuf_b.at[ql], ql, 1, (1, 0), b_done)

    with jax.named_scope("farwait"):
        for b in range(nh):
            for d in range(2):
                part = mu_all.at[fit, span(far, d * kh + b * KB, KB)]
                pltpu.make_async_copy(part, part, far_recv.at[d, b]).wait()
                k = 7 + d * nh + b
                push(far, d * kh + b * KB, KB, sib_send.at[k], sib_recv.at[k], sib)
    ofit = lax.rem(fit + 1, fits)

    def sib_wait(x, start, size, k):
        part = mu_all.at[ofit, span(x, start, size)]
        pltpu.make_async_copy(part, part, sib_recv.at[k]).wait()

    with jax.named_scope("sibwait"):
        sib_wait(xi, 0, kd, 2)
        for d, x in ((0, left), (1, right)):
            sib_wait(x, d * kh, kh, d)
            sib_wait(x, (1 - d) * kh, kh // 2, 3 + 2 * d)
            sib_wait(x, (1 - d) * kh + kh // 2, kh // 2, 4 + 2 * d)
            for b in range(nh):
                sib_wait(far, d * kh + b * KB, KB, 7 + d * nh + b)

    part = small_buf.at[pl.ds(0, n_row - 1)]
    pltpu.make_async_copy(part, part, sm_recv).wait()
    pltpu.make_async_copy(part, part, sm_send).wait()
    for w in waits:
        w()
    def drain(t, c):
        for q in range(nx):
            stat_wait(t, q, True)
        return c
    lax.fori_loop(0, sweeps, drain, 0)
    for cpy in x_copies:
        cpy.wait_send()
    for d in range(2):
        bulk_copy(d, left, 0).wait_send()
        bulk_copy(d, left, 1).wait_send()
        a_copy(d, left).wait_send()


def finish_kernel(fits, mu_all, small, o_mu, o_logpi, o_lse, logpi_buf, lse_buf, sems):
    row = lax.axis_index("row")
    fit = lax.rem(row, fits)
    first = row - fit
    n_row = small.shape[0]
    nx = n_row // fits
    kd = o_logpi.shape[1] // nx
    per = o_lse.shape[1] // LANES
    parts = 4
    step = mu_all.shape[1] // parts
    copies = []
    for f in range(fits):
        for p in range(parts):
            part = pl.ds(p * step, step)
            copies.append(pltpu.make_async_copy(mu_all.at[f, part], o_mu.at[f, part], sems.at[f * parts + p]))
            copies[-1].start()
    for f in range(fits):
        for j in range(per):
            v = small[first + f, 1, j:j + 1, :]
            for g in range(1, fits):
                v = jnp.where(fit == g, small[first + f, 1, g * per + j:g * per + j + 1, :], v)
            lse_buf[f:f + 1, j * LANES:(j + 1) * LANES] = v
        for x in range(nx):
            for j in range(kd // LANES):
                logpi_buf[f:f + 1, x * kd + j * LANES:x * kd + (j + 1) * LANES] = small[x * fits + f, 0, j:j + 1, :]
    n = fits * parts
    for k, (src, dst) in enumerate(((logpi_buf, o_logpi), (lse_buf, o_lse))):
        copies.append(pltpu.make_async_copy(src, dst, sems.at[n + k]))
        copies[-1].start()
    for c in copies:
        c.wait()


def solution(mesh):
    comp_size = mesh.shape["comp"]
    row_size = mesh.shape["row"]

    def local_fit(x_local, mu_init, logpi_init, inv_temp):
        n_rows, full_dim = x_local.shape
        fits, n_local, half = mu_init.shape
        sweeps = inv_temp.shape[0]
        nx = row_size // fits
        kd = n_local // nx
        cp = n_rows * fits
        n_peer = comp_size * nx
        kb = LANES
        nh = kd // 2 // kb
        dims = {"fits": fits, "comp": comp_size, "row": row_size, "sweeps": sweeps}
        f32, bf16 = jnp.float32, jnp.bfloat16
        dma = pltpu.SemaphoreType.DMA
        srows = cp // LANES
        hbm = pl.BlockSpec(memory_space=pltpu.HBM)
        vmem = pl.BlockSpec(memory_space=pltpu.VMEM)
        mu, small = pl.pallas_call(
            functools.partial(em_kernel, dims),
            out_shape=(pltpu.VMEM((fits, n_local, half), f32),
                       pltpu.VMEM((row_size, 2, kd // LANES, LANES), f32)),
            in_specs=[hbm] * 4,
            out_specs=(vmem, vmem),
            scratch_shapes=[
                pltpu.SMEM((sweeps,), f32),
                pltpu.VMEM((n_rows, full_dim), bf16),
                pltpu.VMEM((fits, n_local), f32),
                pltpu.VMEM((nx, cp, half), bf16),
                pltpu.VMEM((kd, half), f32),
                pltpu.VMEM((kd, half), bf16),
                pltpu.VMEM((kd, LANES), f32),
                pltpu.VMEM((nx, kd, cp), f32),
                pltpu.VMEM((kd, cp), bf16),
                pltpu.VMEM((kd, half), f32),
                pltpu.VMEM((kd, LANES), f32),
                pltpu.VMEM((sweeps, nx, 2, srows, LANES), f32),
                pltpu.VMEM((sweeps, nx, n_peer, 2, srows, LANES), f32),
                pltpu.VMEM((nx, 8, cp), f32),
                pltpu.VMEM((2, kd // LANES, LANES), f32),
                pltpu.VMEM((kd // LANES, LANES), f32),
                pltpu.VMEM((2, kd, half), bf16),
                pltpu.VMEM((2, kd // LANES, LANES), f32),
                pltpu.VMEM((2, kd, LANES), f32),
                pltpu.VMEM((nx, 2, kd // 2, cp), f32),
                pltpu.VMEM((nx, 2, kd // 2, cp), f32),
                pltpu.VMEM((nx, 2, kd // 2, cp), bf16),
                pltpu.VMEM((2, 2, kd // 2, half), f32),
                pltpu.VMEM((2, 2, kd // 2, LANES), f32),
                dma((4,)), dma, dma((nx,)),
                dma((sweeps, nx)), dma((sweeps, nx)),
                dma, dma,
                dma((2, 2)), dma((2, 2)), dma((2,)), dma((2,)),
                dma((2, nh)), dma((2, nh)), dma((7 + 2 * nh,)), dma((7 + 2 * nh,)),
            ],
            compiler_params=pltpu.CompilerParams(collective_id=0, has_side_effects=True,
                                                 vmem_limit_bytes=48 * 1024 * 1024),
        )(*[pltpu.with_memory_space_constraint(v, pltpu.HBM) for v in (inv_temp, x_local, mu_init, logpi_init)])
        return pl.pallas_call(
            functools.partial(finish_kernel, fits),
            out_shape=(jax.ShapeDtypeStruct((fits, n_local, half), f32),
                       jax.ShapeDtypeStruct((fits, n_local), f32),
                       jax.ShapeDtypeStruct((fits, n_rows), f32)),
            in_specs=[pl.BlockSpec(memory_space=pl.ANY), vmem],
            out_specs=(hbm, hbm, hbm),
            scratch_shapes=[pltpu.VMEM((fits, n_local), f32), pltpu.VMEM((fits, n_rows), f32), dma((4 * fits + 2,))],
            compiler_params=pltpu.CompilerParams(vmem_limit_bytes=8 * 1024 * 1024),
        )(pltpu.with_memory_space_constraint(mu, pltpu.VMEM), pltpu.with_memory_space_constraint(small, pltpu.VMEM))

    return jax.shard_map(
        local_fit,
        mesh=mesh,
        in_specs=(P(("grp", "row"), None), P(None, ("grp", "comp"), None), P(None, ("grp", "comp")), P()),
        out_specs=(P(None, ("grp", "comp"), None), P(None, ("grp", "comp")), P(None, ("grp", "row"))),
        check_vma=False,
    )
```
